32 devices in a mesh: dom: 32 (over z, y, x, core).
Axes of the slice: x: 2, y: 2, z: 4, core: 2. Of those that a mesh axis runs over, the one named last changes fastest.
Arguments:
- features: bfloat16 [524288, 256], P('dom'), may hold values from -48 to 48, as said below
- w_first: bfloat16 [1280, 256], replicated, may hold values from -0.15625 to 0.15625
- w_second: bfloat16 [1280, 256], replicated, may hold values from -0.15625 to 0.15625
- seed_owner: int32 [9216, 1], P('dom'), may hold values from 0 to 31; in each aligned block of 288 rows (0 to 287, 288 to 575, ...) at most 18 rows name the same one
- seed_row: int32 [9216], P('dom'), may hold values from 0 to 16383
- hop1_owner: int32 [36864, 1], P('dom'), may hold values from 0 to 31; in each aligned block of 1152 rows (0 to 1151, 1152 to 2303, ...) at most 72 rows name the same one
- hop1_row: int32 [36864], P('dom'), may hold values from 0 to 16383
- hop1_rel: int32 [36864], P('dom'), may hold values from 0 to 3
- hop2_owner: int32 [73728, 1], P('dom'), may hold values from 0 to 31; in each aligned block of 2304 rows (0 to 2303, 2304 to 4607, ...) at most 144 rows name the same one
- hop2_row: int32 [73728], P('dom'), may hold values from 0 to 16383
- hop2_rel: int32 [73728], P('dom'), may hold values from 0 to 3
- edge_mask: int32 [4096], P('dom'), may hold values 0 or 1
Outputs:
- edge_loss: float32 [4096], P('dom')
- mean_loss: float32 [], replicated
The draws below stay inside these ranges and needn't reach their ends.
Inputs may be any that keep to these rules, and one draw needn't show every extreme that they name: `features`: standard normal entries; in some draws each row is scaled by a factor up to 10. `seed_owner`: among the rows of one device no owner is named by more than 18 rows; some owner is named by exactly 18 in every draw. `hop1_owner`: among the rows of one device no owner is named by more than 72 rows; some owner is named by exactly 72 in every draw. `hop2_owner`: among the rows of one device no owner is named by more than 144 rows; some owner is named by exactly 144 in every draw.
All inputs are finite; a program needn't handle non-finite values. No bound on the sum of `edge_mask` on one device may be relied on, other than what follows from the above.
Results may differ from the reference program's by a relative error of at most 0.002.
Values may be sent and summed in bfloat16 or wider, within the bound.
A program may use at most 64 MiB of HBM per device.

```python
import math
import jax
import jax.numpy as jnp
import numpy as np
from jax import lax

F = 256
R = 4
NODE_DEV = 16384
POS_DEV = 128
BLOCK = 128
NEG = 32
FAN1 = 4
FAN2 = 2
BLOCKS_DEV = 1
SEED_DEV = 288
H1_DEV = 1152
H2_DEV = 2304
CAP_S = 18
CAP_1 = 72
CAP_2 = 144
NODES = 524288
EDGES = 4096
SEEDS = 9216
H1 = 36864
H2 = 73728
N_DOM = 32


def draw_features(key, part):
    first_key = jax.random.fold_in(key, 0)
    values = jax.random.normal(first_key, (NODES, F), jnp.float32)
    values = jnp.clip(values, -6.0, 6.0)
    return values.astype(jnp.bfloat16)


def place_ends(array, rng, low, high):
    longest = array.shape.index(max(array.shape))
    spots = []
    for shift in (0, 1):
        where = [jax.random.randint(jax.random.fold_in(rng, axis), (), 0, length) for axis, length in enumerate(array.shape)]
        where[longest] = (where[longest] + shift) % array.shape[longest]
        spots.append(tuple(where))
    return array.at[spots[0]].set(low).at[spots[1]].set(high)


def shared_out(rng, own, number, rows, number_of, top, bound, skew):
    sequence = jax.random.permutation(rng, number_of)
    heavy_load, common = portions_of(number_of, rows * top, bound, skew, True), portions_of(number_of, rows * top, bound, skew, False)
    places = jnp.arange(number_of)

    def named(sizes, turn):
        used = int((sizes > 0).sum())
        fixed = max(1, used // 4)
        shifted = fixed + (places - fixed + turn * (used - fixed)) % max(1, number_of - fixed)
        return jnp.zeros((number_of,), jnp.int32).at[sequence[jnp.where(places < fixed, places, shifted)]].set(jnp.asarray(sizes, jnp.int32))

    sizes = jnp.where(number % 4 == 0, named(heavy_load, number // 4), named(common, number - number // 4 - 1))
    mixed = jax.random.permutation(jax.random.fold_in(own, 3), number_of)
    donor, taker = mixed[0:number_of // 2 * 2:2], mixed[1:number_of // 2 * 2:2]
    slack = jnp.minimum(sizes[donor] - 1, bound - sizes[taker]) // 2
    slack = jnp.where((donor == sequence[0]) | (taker == sequence[0]) | (sizes[taker] == 0), 0, jnp.maximum(slack, 0))
    shifted = jax.random.randint(jax.random.fold_in(own, 4), (number_of // 2,), 0, 1 << 20) % (slack + 1)
    sizes = sizes.at[donor].add(-shifted).at[taker].add(shifted)
    members = jnp.searchsorted(jnp.cumsum(sizes), jnp.arange(rows * top), side="right").astype(jnp.int32)
    grid = members.reshape(top, rows).T
    grid = grid[jax.random.permutation(jax.random.fold_in(own, 1), rows)]
    turn = jax.random.randint(jax.random.fold_in(own, 2), (rows, 1), 0, top)
    return jnp.take_along_axis(grid, (jnp.arange(top)[None, :] + turn) % top, axis=1)


def portions_of(amount, total, reach, lean, full):
    loads = [(1 << 20) // math.isqrt(standing ** lean) + 1 for standing in range(1, amount + 1)]
    largest = reach if full else min(reach, max(-(-total // amount), total * loads[0] // sum(loads)))
    least = 1 if total - largest >= amount - 1 else 0
    given, spare = [largest] + [least] * (amount - 1), total - largest - least * (amount - 1)
    while spare > 0:
        movable = [i for i in range(1, amount) if given[i] < largest] or [i for i in range(1, amount) if given[i] < reach]
        mass, remaining = sum([loads[i] for i in movable]), spare
        for i in movable:
            more = min(reach - given[i], max(1, remaining * loads[i] // mass), spare)
            given[i] = given[i] + more
            spare = spare - more
    return np.array(given)


def noise(rng, extent, scale, most, held_as=jnp.bfloat16):
    return jnp.clip(scale * jax.random.normal(rng, extent, jnp.float32), -most, most).astype(held_as)


def setup_inputs(seed: int = 0) -> dict:
    splits = jax.random.split(jax.random.key(seed), 13)
    features = draw_features(jax.random.fold_in(splits[12], 71), 0)
    w_first = noise(splits[1], ((R + 1) * F, F), ((R + 1) * F) ** -0.5, 0.15625)
    w_second = noise(splits[2], ((R + 1) * F, F), ((R + 1) * F) ** -0.5, 0.15625)
    seed_owner_keys = jax.random.split(jax.random.fold_in(splits[3], 1), SEEDS // SEED_DEV)
    seed_owner_turns = jax.random.permutation(jax.random.fold_in(splits[3], 3), SEEDS // SEED_DEV)
    seed_owner = jax.vmap(lambda own, number: shared_out(jax.random.fold_in(splits[3], 2), own, number, SEED_DEV, N_DOM, 1, CAP_S, 2))(seed_owner_keys, seed_owner_turns).reshape((SEEDS, 1))
    seed_row = place_ends(jax.random.randint(splits[4], (SEEDS,), 0, NODE_DEV), jax.random.fold_in(splits[4], 1), 0, NODE_DEV - 1).astype(jnp.int32)
    hop1_owner_keys = jax.random.split(jax.random.fold_in(splits[5], 1), H1 // H1_DEV)
    hop1_owner_turns = jax.random.permutation(jax.random.fold_in(splits[5], 3), H1 // H1_DEV)
    hop1_owner = jax.vmap(lambda own, number: shared_out(jax.random.fold_in(splits[5], 2), own, number, H1_DEV, N_DOM, 1, CAP_1, 2))(hop1_owner_keys, hop1_owner_turns).reshape((H1, 1))
    hop1_row = place_ends(jax.random.randint(splits[6], (H1,), 0, NODE_DEV), jax.random.fold_in(splits[6], 1), 0, NODE_DEV - 1).astype(jnp.int32)
    hop1_rel = place_ends(jax.random.randint(splits[7], (H1,), 0, R), jax.random.fold_in(splits[7], 1), 0, R - 1).astype(jnp.int32)
    hop2_owner_keys = jax.random.split(jax.random.fold_in(splits[8], 1), H2 // H2_DEV)
    hop2_owner_turns = jax.random.permutation(jax.random.fold_in(splits[8], 3), H2 // H2_DEV)
    hop2_owner = jax.vmap(lambda own, number: shared_out(jax.random.fold_in(splits[8], 2), own, number, H2_DEV, N_DOM, 1, CAP_2, 2))(hop2_owner_keys, hop2_owner_turns).reshape((H2, 1))
    hop2_row = place_ends(jax.random.randint(splits[9], (H2,), 0, NODE_DEV), jax.random.fold_in(splits[9], 1), 0, NODE_DEV - 1).astype(jnp.int32)
    hop2_rel = place_ends(jax.random.randint(splits[10], (H2,), 0, R), jax.random.fold_in(splits[10], 1), 0, R - 1).astype(jnp.int32)
    edge_mask = place_ends((jax.random.randint(splits[11], (EDGES,), 0, 4) < 3).astype(jnp.int32), jax.random.fold_in(splits[11], 1), 0, 1)
    return dict(features=features, w_first=w_first, w_second=w_second, seed_owner=seed_owner, seed_row=seed_row, hop1_owner=hop1_owner, hop1_row=hop1_row, hop1_rel=hop1_rel, hop2_owner=hop2_owner, hop2_row=hop2_row, hop2_rel=hop2_rel, edge_mask=edge_mask)


def rgcn_layer(self_rows, neighbours, relations, weights):
    onehot = (relations[..., None] == jnp.arange(R, dtype=jnp.int32)).astype(jnp.float32)
    tallies = jnp.maximum(jnp.sum(onehot, axis=1), 1.0)
    shares = onehot / tallies[:, None, :]
    merged = jnp.einsum('nkr,nkf->nrf', shares, neighbours.astype(jnp.float32)).astype(jnp.bfloat16)
    inputs = jnp.concatenate([self_rows, merged.reshape(self_rows.shape[0], R * F)], axis=1)
    return jnp.dot(inputs, weights, preferred_element_type=jnp.float32)


def edge_scores(second):
    sources = second[:POS_DEV]
    targets = second[POS_DEV:2 * POS_DEV]
    negatives = second[2 * POS_DEV:].reshape(BLOCKS_DEV, NEG, F)
    positive = jnp.sum(sources * targets, axis=1)
    negative = jnp.einsum('bef,bqf->beq', sources.reshape(BLOCKS_DEV, BLOCK, F), negatives,
                          precision=lax.Precision.HIGHEST).reshape(POS_DEV, NEG)
    scores = jnp.concatenate([positive[:, None], negative], axis=1)
    top_score = jnp.max(scores, axis=1, keepdims=True)
    return top_score[:, 0] + jnp.log(jnp.sum(jnp.exp(scores - top_score), axis=1)) - positive


def reference(features, w_first, w_second, seed_owner, seed_row, hop1_owner, hop1_row, hop1_rel,
              hop2_owner, hop2_row, hop2_rel, edge_mask):
    def one_device(pieces):
        s_owner, s_row, a_owner, a_row, a_rel, b_owner, b_row, b_rel = pieces
        x_seed = features[(s_owner * NODE_DEV + s_row).astype(jnp.int32)]
        x_hop1 = features[(a_owner * NODE_DEV + a_row).astype(jnp.int32)]
        x_hop2 = features[(b_owner * NODE_DEV + b_row).astype(jnp.int32)]
        first_hop = jax.nn.relu(rgcn_layer(x_hop1, x_hop2.reshape(H1_DEV, FAN2, F),
                                           b_rel.reshape(H1_DEV, FAN2), w_first)).astype(jnp.bfloat16)
        first_seed = jax.nn.relu(rgcn_layer(x_seed, x_hop1.reshape(SEED_DEV, FAN1, F),
                                            a_rel.reshape(SEED_DEV, FAN1), w_first)).astype(jnp.bfloat16)
        second = rgcn_layer(first_seed, first_hop.reshape(SEED_DEV, FAN1, F),
                            a_rel.reshape(SEED_DEV, FAN1), w_second)
        return edge_scores(second)

    pieces = (seed_owner.reshape(N_DOM, SEED_DEV), seed_row.reshape(N_DOM, SEED_DEV),
              hop1_owner.reshape(N_DOM, H1_DEV), hop1_row.reshape(N_DOM, H1_DEV),
              hop1_rel.reshape(N_DOM, H1_DEV), hop2_owner.reshape(N_DOM, H2_DEV),
              hop2_row.reshape(N_DOM, H2_DEV), hop2_rel.reshape(N_DOM, H2_DEV))
    edge_loss = lax.map(one_device, pieces).reshape(EDGES)
    weights = edge_mask.astype(jnp.float32)
    mean_loss = jnp.sum(weights * edge_loss) / jnp.maximum(jnp.sum(weights), 1.0)
    return edge_loss, mean_loss
```

```python
import functools

import jax
import jax.numpy as jnp
from jax import lax
from jax.experimental import pallas as pl
from jax.experimental.pallas import tpu as pltpu
from jax.sharding import PartitionSpec as P

MESH = pl.DeviceIdType.MESH
HOP = 11
PIECE = 96
LANES = 128
LOADS = 8
UNROLL = 24

R = 4
BLOCK = 128
NEG = 32
FAN1 = 4
FAN2 = 2

HALF, FULL = jnp.bfloat16, jnp.float32


def round_up(value, multiple):
    return (value + multiple - 1) // multiple * multiple


def unroll_of(count, most=UNROLL):
    return max(step for step in range(1, most + 1) if count % step == 0)


def greet(devices, me):
    barrier = pltpu.get_barrier_semaphore()

    def hail(step, carry):
        other = lax.rem(me + step, devices)
        pl.semaphore_signal(barrier, inc=1, device_id=(other,), device_id_type=MESH)
        return carry

    lax.fori_loop(1, devices, hail, 0)
    return lambda: pl.semaphore_wait(barrier, devices - 1)


def gather_rows(table, index_of, count, staging):
    step = unroll_of(count)

    def some(turn, carry):
        for lane in range(step):
            place = turn * step + lane
            staging[pl.ds(place, 1), :] = table[pl.ds(index_of(place), 1), :]
        return carry

    lax.fori_loop(0, count // step, some, 0)


def ranks(devices, owner_ref, blocks):
    lane = lax.broadcasted_iota(jnp.int32, (LANES, 2 * LANES), 1)
    item = lax.broadcasted_iota(jnp.int32, (LANES, 2 * LANES), 0)
    counting = ((item < lane) | (lane >= LANES)).astype(HALF)
    owner_id = lax.broadcasted_iota(jnp.int32, (devices, LANES), 0)
    hots = []
    for block in range(blocks):
        owner = owner_ref[0:1, block * LANES : (block + 1) * LANES]
        hots.append((owner == owner_id).astype(FULL))
    counted = jnp.dot(
        jnp.concatenate(hots, axis=0).astype(HALF), counting, preferred_element_type=FULL
    )
    running = jnp.zeros((devices, LANES), FULL)
    positions = []
    for block in range(blocks):
        mine = counted[block * devices : (block + 1) * devices]
        prior = mine[:, :LANES] + running
        running = running + mine[:, LANES:]
        positions.append(jnp.sum(prior * hots[block], axis=0, keepdims=True))
    return hots, positions


def asked_of(hots, positions, rows_ref, offset, width):
    slot = lax.broadcasted_iota(jnp.int32, (width, LANES), 0).astype(FULL)
    total = None
    for block, (hot, position) in enumerate(zip(hots, positions)):
        row = rows_ref[block : block + 1, :]
        high = lax.shift_right_logical(row, 7).astype(FULL)
        low = jnp.bitwise_and(row, 127).astype(FULL)
        digits = jnp.concatenate([hot * high, hot * low], axis=0).astype(HALF)
        placed = (slot == position + float(offset)).astype(FULL).astype(HALF)
        term = lax.dot_general(
            digits, placed, (((1,), (1,)), ((), ())), preferred_element_type=FULL
        )
        total = term if total is None else total + term
    return total


def shares_of(kinds, fan):
    first = lax.broadcasted_iota(jnp.int32, (LANES, LANES), 0) // fan
    second = lax.broadcasted_iota(jnp.int32, (LANES, LANES), 1) // fan
    together = (first == second).astype(HALF)
    count = None
    for kind in range(R):
        same = (kinds == kind).astype(FULL)
        term = same * jnp.dot(same.astype(HALF), together, preferred_element_type=FULL)
        count = term if count is None else count + term
    return 1.0 / jnp.maximum(count, 1.0)


def fetch_kernel(
    devices,
    caps,
    strides,
    counts,
    far_owner,
    first_owner,
    seed_owner,
    far_row,
    first_row,
    seed_row,
    far_kind,
    first_kind,
    features,
    w_first,
    w_second,
    near_kinds,
    mask,
    loss_out,
    mean_out,
    table_half,
    table,
    asks,
    requests,
    arrived,
    wanted,
    look_own,
    look_out,
    look_in,
    share_own,
    share_in,
    look,
    share,
    far_send,
    near_send,
    far_recv,
    near_recv,
    far_cast,
    near_cast,
    staging,
    layer,
    piece_send,
    piece_recv,
    second,
    part,
    seen,
    load_sem,
    small_sem,
    ask_send,
    ask_recv,
    info_send,
    info_recv,
    far_send_sem,
    far_recv_sem,
    near_send_sem,
    near_recv_sem,
    piece_send_sem,
    piece_recv_sem,
    tell_send,
    tell_recv,
):
    me = lax.axis_index("dom")
    side = devices // 2
    half = lax.div(me, side)
    local = lax.rem(me, side)
    mirror = lax.rem(me + side, devices)
    far_count, first_count, seed_count = counts
    width = table.shape[1]
    far_cap, first_cap, seed_cap = caps
    far_stride, near_stride = strides
    far_rows, near_rows = side * far_stride, side * near_stride
    asked = requests.shape[2]
    chunk = table.shape[0] // LOADS
    loads = []
    for turn in range(LOADS):
        where = pl.ds(turn * chunk, chunk)
        loads.append(
            pltpu.make_async_copy(features.at[where], table_half.at[where], load_sem.at[turn])
        )
        loads[-1].start()
    met = greet(devices, me)

    far_blocks, first_blocks, seed_blocks = (
        far_row.shape[0],
        first_row.shape[0],
        seed_row.shape[0],
    )
    far_hot, far_pos = ranks(devices, far_owner, far_blocks)
    first_hot, first_pos = ranks(devices, first_owner, first_blocks)
    seed_hot, seed_pos = ranks(devices, seed_owner, seed_blocks)
    digits = (
        asked_of(far_hot, far_pos, far_row, 0, asked)
        + asked_of(first_hot, first_pos, first_row, far_stride, asked)
        + asked_of(seed_hot, seed_pos, seed_row, far_stride + first_cap, asked)
    )
    wishes = (digits[:devices] * 128.0 + digits[devices:]).astype(jnp.int32)
    asks[...] = jnp.clip(wishes, 0, table.shape[0] - 1)

    def lay(owner, carry):
        requests[owner] = asks[pl.ds(owner, 1), :]
        return carry

    lax.fori_loop(0, devices, lay, 0)
    met()

    def ask(turn, carry):
        other = lax.rem(me + turn * HOP, devices)
        pltpu.make_async_remote_copy(
            src_ref=requests.at[other],
            dst_ref=arrived.at[me],
            send_sem=ask_send,
            recv_sem=ask_recv,
            device_id=(other,),
            device_id_type=MESH,
        ).start()
        return carry

    lax.fori_loop(1, devices, ask, 0)
    own_ask = pltpu.make_async_copy(requests.at[me], arrived.at[me], small_sem.at[0])
    own_ask.start()

    far_base = 0
    first_base = far_blocks * LANES
    turn_base = first_base + first_blocks * LANES
    seed_base = turn_base + first_blocks * LANES
    far_zero, near_zero = R * far_rows, (R + 1) * near_rows

    def place_of(position, cap):
        return jnp.clip(position.astype(jnp.int32), 0, cap - 1)

    def put(base, block, owner, place, kind, rows, stride, zero):
        lanes = slice(base + block * LANES, base + (block + 1) * LANES)
        for ref, whose in ((look_own, half), (look_out, 1 - half)):
            at = owner - whose * side
            held = (at >= 0) & (at < side)
            index = at * stride + place
            if kind is not None:
                index = index + kind * rows
            ref[0:1, lanes] = jnp.where(held, index, zero)

    for block in range(far_blocks):
        owner = far_owner[0:1, block * LANES : (block + 1) * LANES]
        place = place_of(far_pos[block], far_cap)
        kind = far_kind[block : block + 1, :]
        put(far_base, block, owner, place, kind, far_rows, far_stride, far_zero)
    for block in range(first_blocks):
        owner = first_owner[0:1, block * LANES : (block + 1) * LANES]
        place = place_of(first_pos[block], first_cap)
        kind = first_kind[block : block + 1, :] + 1
        put(first_base, block, owner, place, None, near_rows, near_stride, near_zero)
        put(turn_base, block, owner, place, kind, near_rows, near_stride, near_zero)
    for block in range(seed_blocks):
        owner = seed_owner[0:1, block * LANES : (block + 1) * LANES]
        place = place_of(seed_pos[block], seed_cap) + first_cap
        put(seed_base, block, owner, place, None, near_rows, near_stride, near_zero)
    far_share = shares_of(far_kind[...], FAN2)
    first_share = shares_of(first_kind[...], FAN1)
    for block in range(far_blocks):
        share_own[0:1, block * LANES : (block + 1) * LANES] = far_share[block : block + 1, :]
    for block in range(first_blocks):
        lanes = slice(first_base + block * LANES, first_base + (block + 1) * LANES)
        share_own[0:1, lanes] = first_share[block : block + 1, :]
    tells = []
    for turn, (source, target) in enumerate(((look_out, look_in), (share_own, share_in))):
        tells.append(
            pltpu.make_async_remote_copy(
                src_ref=source,
                dst_ref=target,
                send_sem=info_send.at[turn],
                recv_sem=info_recv.at[turn],
                device_id=(mirror,),
                device_id_type=MESH,
            )
        )
        tells[-1].start()
    keeps = [
        pltpu.make_async_copy(look_own, look.at[0], small_sem.at[1]),
        pltpu.make_async_copy(share_own, share.at[0], small_sem.at[2]),
    ]
    for keep in keeps:
        keep.start()

    part_rows = chunk // 4
    for turn in range(LOADS):
        loads[turn].wait()

        def widen(quarter, carry):
            start = pl.multiple_of(turn * chunk + quarter * part_rows, part_rows)
            where = pl.ds(start, part_rows)
            table[where, :] = table_half[where, :].astype(FULL)
            return carry

        lax.fori_loop(0, 4, widen, 0)
    own_ask.wait()
    others = pl.ds(0, devices - 1)
    pltpu.make_async_copy(requests.at[others], arrived.at[others], ask_send).wait()
    pltpu.make_async_copy(requests.at[others], arrived.at[others], ask_recv).wait()
    move = pltpu.make_async_copy(arrived, wanted, small_sem.at[0])
    move.start()
    move.wait()

    def serve(first, stride, send, recv, turn, send_sem, recv_sem):
        whose = lax.rem(half + turn, 2) * side
        where = pl.ds(pl.multiple_of(local * stride, stride), stride)

        def pick(other):
            gather_rows(table, lambda place: wanted[other, 0, first + place], stride, staging)
            return staging[pl.ds(0, stride), :].astype(HALF)

        def one(step, carry):
            relay = lax.rem(local + step * HOP, side)
            client = whose + relay
            send[client] = pick(client)
            pltpu.make_async_remote_copy(
                src_ref=send.at[client],
                dst_ref=recv.at[turn, where],
                send_sem=send_sem.at[turn],
                recv_sem=recv_sem.at[turn],
                device_id=(half * side + relay,),
                device_id_type=MESH,
            ).start()
            return carry

        lax.fori_loop(1, side, one, 0)
        recv[turn, where, :] = pick(whose + local)

    for turn in (1, 0):
        serve(0, far_stride, far_send, far_recv, turn, far_send_sem, far_recv_sem)
        serve(far_stride, near_stride, near_send, near_recv, turn, near_send_sem, near_recv_sem)

    far_cast[far_zero : far_zero + 8, :] = jnp.zeros((8, width), FULL)
    near_cast[near_zero : near_zero + 8, :] = jnp.zeros((8, width), FULL)

    for tell in tells:
        tell.wait()
    keeps += [
        pltpu.make_async_copy(look_in, look.at[1], small_sem.at[3]),
        pltpu.make_async_copy(share_in, share.at[1], small_sem.at[4]),
    ]
    for keep in keeps[2:]:
        keep.start()
    for keep in keeps:
        keep.wait()

    def arrive(recv, turn, rows, stride, recv_sem):
        there = pl.ds(0, rows - stride)
        block = recv.at[turn, there]
        pltpu.make_async_copy(block, block, recv_sem.at[turn]).wait()

    def project(recv, turn, rows, cast, first_kind_of, kinds):
        size = rows // 2

        def some(part_of, carry):
            start = pl.multiple_of(part_of * size, size)
            values = recv[turn, pl.ds(start, size), :]
            for kind in range(kinds):
                top = (first_kind_of + kind) * width
                target = pl.ds(pl.multiple_of(kind * rows + start, 8), size)
                cast[target, :] = jnp.dot(
                    values, w_first[top : top + width, :], preferred_element_type=FULL
                )
            return carry

        lax.fori_loop(0, 2, some, 0)

    def hop_rows(turn, fan, start, target, offset):
        step = unroll_of(PIECE, 16)

        def some(count, carry):
            for lane in range(step):
                place = count * step + lane
                item = (start + place) * FAN1 + fan
                pair = item * FAN2
                total = far_cast[pl.ds(look[turn, 0, far_base + pair], 1), :]
                for k in range(1, FAN2):
                    total = total + far_cast[pl.ds(look[turn, 0, far_base + pair + k], 1), :]
                own = near_cast[pl.ds(look[turn, 0, first_base + item], 1), :]
                target[pl.ds(offset + place, 1), :] = own + share[turn, 0, pair] * total
            return carry

        lax.fori_loop(0, PIECE // step, some, 0)

    def seed_rows(turn, start, target, offset):
        step = unroll_of(PIECE, 12)

        def some(count, carry):
            for lane in range(step):
                place = count * step + lane
                seed = start + place
                total = near_cast[pl.ds(look[turn, 0, seed_base + seed], 1), :]
                for k in range(FAN1):
                    item = seed * FAN1 + k
                    value = near_cast[pl.ds(look[turn, 0, turn_base + item], 1), :]
                    total = total + share[turn, 0, first_base + item] * value
                target[pl.ds(offset + place, 1), :] = total
            return carry

        lax.fori_loop(0, PIECE // step, some, 0)

    each = seed_count // PIECE

    def post(number):
        piece_send[number] = staging[pl.ds(0, PIECE), :].astype(HALF)
        pltpu.make_async_remote_copy(
            src_ref=piece_send.at[number],
            dst_ref=piece_recv.at[number],
            send_sem=piece_send_sem,
            recv_sem=piece_recv_sem,
            device_id=(mirror,),
            device_id_type=MESH,
        ).start()

    arrive(far_recv, 1, far_rows, far_stride, far_recv_sem)
    project(far_recv, 1, far_rows, far_cast, 1, R)
    arrive(near_recv, 1, near_rows, near_stride, near_recv_sem)
    project(near_recv, 1, near_rows, near_cast, 0, R + 1)

    def mirror_hop(number, carry):
        hop_rows(1, number // each, lax.rem(number, each) * PIECE, staging, 0)
        post(number)
        return carry

    lax.fori_loop(0, FAN1 * each, mirror_hop, 0)

    def mirror_seed(number, carry):
        seed_rows(1, number * PIECE, staging, 0)
        post(FAN1 * each + number)
        return carry

    lax.fori_loop(0, each, mirror_seed, 0)

    arrive(far_recv, 0, far_rows, far_stride, far_recv_sem)
    project(far_recv, 0, far_rows, far_cast, 1, R)
    arrive(near_recv, 0, near_rows, near_stride, near_recv_sem)
    project(near_recv, 0, near_rows, near_cast, 0, R + 1)

    def own_hop(number, carry):
        start = lax.rem(number, each) * PIECE
        hop_rows(0, number // each, start, layer, number * PIECE)
        return carry

    lax.fori_loop(0, FAN1 * each, own_hop, 0)

    def own_seed(number, carry):
        seed_rows(0, number * PIECE, layer, first_count + number * PIECE)
        return carry

    lax.fori_loop(0, each, own_seed, 0)

    pieces = (FAN1 + 1) * each
    pltpu.make_async_copy(piece_recv, piece_recv, piece_recv_sem).wait()

    def join(number, carry):
        where = pl.ds(pl.multiple_of(number * PIECE, PIECE), PIECE)
        value = jnp.maximum(layer[where, :] + piece_recv[number].astype(FULL), 0.0)
        layer[where, :] = value.astype(HALF).astype(FULL)
        return carry

    lax.fori_loop(0, pieces, join, 0)

    def weighed(values, kinds, weights):
        fan = len(values)
        hot = [
            [(kinds[:, k : k + 1] == kind).astype(FULL) for k in range(fan)] for kind in range(R)
        ]
        result = None
        for kind in range(R):
            portion = 1.0 / jnp.maximum(sum(hot[kind][1:], hot[kind][0]), 1.0)
            mean = (hot[kind][0] * portion) * values[0]
            for k in range(1, fan):
                mean = mean + (hot[kind][k] * portion) * values[k]
            term = jnp.dot(
                mean.astype(HALF),
                weights[(kind + 1) * width : (kind + 2) * width, :],
                preferred_element_type=FULL,
            )
            result = term if result is None else result + term
        return result

    def seed_piece(turn, carry):
        start = pl.multiple_of(turn * PIECE, PIECE)
        where = pl.ds(start, PIECE)
        values = [
            layer[pl.ds(pl.multiple_of(k * seed_count + start, PIECE), PIECE), :]
            for k in range(FAN1)
        ]
        own = layer[pl.ds(pl.multiple_of(first_count + start, PIECE), PIECE), :]
        second[where, :] = jnp.dot(
            own.astype(HALF), w_second[:width, :], preferred_element_type=FULL
        ) + weighed(values, near_kinds[where, :], w_second)
        return carry

    lax.fori_loop(0, each, seed_piece, 0)

    blocks = mask.shape[0]
    positives = blocks * BLOCK
    loss_sum = jnp.zeros((1, 1), FULL)
    edge_sum = jnp.zeros((1, 1), FULL)

    def pairs(left, right):
        return lax.dot_general(
            left,
            right,
            (((1,), (1,)), ((), ())),
            precision=lax.Precision.HIGHEST,
            preferred_element_type=FULL,
        )

    for block in range(blocks):
        sources = second[block * BLOCK : (block + 1) * BLOCK, :]
        targets = second[positives + block * BLOCK : positives + (block + 1) * BLOCK, :]
        first_neg = 2 * positives + block * NEG
        negatives = second[first_neg : first_neg + NEG, :]
        positive = pairs(jnp.ones((8, width), FULL), sources * targets)[0:1, :]
        negative = pairs(negatives, sources)
        top_score = jnp.maximum(positive, jnp.max(negative, axis=0, keepdims=True))
        spread_sum = jnp.exp(positive - top_score) + jnp.sum(
            jnp.exp(negative - top_score), axis=0, keepdims=True
        )
        edge_loss = top_score + jnp.log(spread_sum) - positive
        loss_out[block : block + 1, :] = edge_loss
        counted = mask[block : block + 1, :].astype(FULL)
        loss_sum = loss_sum + jnp.sum(counted * edge_loss, axis=1, keepdims=True)
        edge_sum = edge_sum + jnp.sum(counted, axis=1, keepdims=True)
    lane = lax.broadcasted_iota(jnp.int32, (1, LANES), 1)
    part[...] = jnp.where(lane == 0, loss_sum, jnp.where(lane == 1, edge_sum, 0.0))

    def tell_all(turn, carry):
        other = lax.rem(me + turn * HOP, devices)
        pltpu.make_async_remote_copy(
            src_ref=part,
            dst_ref=seen.at[me],
            send_sem=tell_send,
            recv_sem=tell_recv,
            device_id=(other,),
            device_id_type=MESH,
        ).start()
        return carry

    lax.fori_loop(1, devices, tell_all, 0)
    seen[me] = part[...]
    near_side = pl.ds(0, side - 1)
    for turn in range(2):
        sent = far_send.at[near_side]
        pltpu.make_async_copy(sent, sent, far_send_sem.at[turn]).wait()
        sent = near_send.at[near_side]
        pltpu.make_async_copy(sent, sent, near_send_sem.at[turn]).wait()
    pltpu.make_async_copy(piece_send, piece_send, piece_send_sem).wait()
    pltpu.make_async_copy(seen.at[others], seen.at[others], tell_recv).wait()
    pltpu.make_async_copy(seen.at[others], seen.at[others], tell_send).wait()
    total = jnp.sum(seen[...], axis=0)
    mean_out[...] = total[:, 0:1] / jnp.maximum(total[:, 1:2], 1.0)


def fetch(owners, rows, kinds, features, w_first, w_second, near_kinds, mask, caps, counts, devices):
    nodes, width = features.shape
    side = devices // 2
    strides = (round_up(caps[0], 16), round_up(caps[1] + caps[2], 16))
    asked = round_up(sum(strides), LANES)
    far_rows, near_rows = side * strides[0], side * strides[1]
    looks = LANES * (rows[0].shape[0] + 2 * rows[1].shape[0] + rows[2].shape[0])
    shared = LANES * (rows[0].shape[0] + rows[1].shape[0])
    pieces = (counts[1] + counts[2]) // PIECE
    number = jnp.int32
    vmem = pl.BlockSpec(memory_space=pltpu.VMEM)
    return pl.pallas_call(
        functools.partial(fetch_kernel, devices, caps, strides, counts),
        out_shape=[
            jax.ShapeDtypeStruct(mask.shape, FULL),
            jax.ShapeDtypeStruct((1, 1), FULL),
        ],
        in_specs=[vmem] * 8 + [pl.BlockSpec(memory_space=pl.ANY)] + [vmem] * 4,
        out_specs=[vmem, vmem],
        scratch_shapes=[
            pltpu.VMEM((nodes, width), HALF),
            pltpu.VMEM((nodes, width), FULL),
            pltpu.VMEM((devices, asked), number),
            pltpu.VMEM((devices, 1, asked), number),
            pltpu.VMEM((devices, 1, asked), number),
            pltpu.SMEM((devices, 1, asked), number),
            pltpu.VMEM((1, looks), number),
            pltpu.VMEM((1, looks), number),
            pltpu.VMEM((1, looks), number),
            pltpu.VMEM((1, shared), FULL),
            pltpu.VMEM((1, shared), FULL),
            pltpu.SMEM((2, 1, looks), number),
            pltpu.SMEM((2, 1, shared), FULL),
            pltpu.VMEM((devices, strides[0], width), HALF),
            pltpu.VMEM((devices, strides[1], width), HALF),
            pltpu.VMEM((2, far_rows, width), HALF),
            pltpu.VMEM((2, near_rows, width), HALF),
            pltpu.VMEM((R * far_rows + 8, width), FULL),
            pltpu.VMEM(((R + 1) * near_rows + 8, width), FULL),
            pltpu.VMEM((round_up(max(strides[0], strides[1], PIECE), 8), width), FULL),
            pltpu.VMEM((counts[1] + counts[2], width), FULL),
            pltpu.VMEM((pieces, PIECE, width), HALF),
            pltpu.VMEM((pieces, PIECE, width), HALF),
            pltpu.VMEM((counts[2], width), FULL),
            pltpu.VMEM((1, LANES), FULL),
            pltpu.VMEM((devices, 1, LANES), FULL),
            pltpu.SemaphoreType.DMA((LOADS,)),
            pltpu.SemaphoreType.DMA((5,)),
            pltpu.SemaphoreType.DMA(()),
            pltpu.SemaphoreType.DMA(()),
        ]
        + [pltpu.SemaphoreType.DMA((2,))] * 6
        + [pltpu.SemaphoreType.DMA(())] * 4,
        compiler_params=pltpu.CompilerParams(
            collective_id=0, has_side_effects=True, vmem_limit_bytes=67043328
        ),
        name="fetch",
    )(*owners, *rows, *kinds, features, w_first, w_second, near_kinds, mask)


def shards(
    features,
    w_first,
    w_second,
    seed_owner,
    seed_row,
    hop1_owner,
    hop1_row,
    hop1_rel,
    hop2_owner,
    hop2_row,
    hop2_rel,
    edge_mask,
):
    devices = lax.axis_size("dom")
    counts = (hop2_row.shape[0], hop1_row.shape[0], seed_row.shape[0])
    caps = tuple((2 * length + devices - 1) // devices for length in counts)

    def flat(values, filler):
        length = values.shape[0]
        values = values.reshape(1, length)
        spare = round_up(length, LANES) - length
        return jnp.pad(values, ((0, 0), (0, spare)), constant_values=filler) if spare else values

    def stacked(values):
        length = values.shape[0]
        spare = round_up(length, LANES) - length
        values = jnp.pad(values, (0, spare)) if spare else values
        return values.reshape(-1, LANES)

    edge_loss, mean_loss = fetch(
        [flat(owner, -1) for owner in (hop2_owner, hop1_owner, seed_owner)],
        [stacked(row) for row in (hop2_row, hop1_row, seed_row)],
        [stacked(rel) for rel in (hop2_rel, hop1_rel)],
        features,
        w_first,
        w_second,
        hop1_rel.reshape(-1, FAN1),
        edge_mask.reshape(-1, BLOCK),
        caps,
        counts,
        devices,
    )
    return (edge_loss.reshape(-1), mean_loss[0, 0])


def solution(mesh):
    placed = (
        P("dom", None),
        P(),
        P(),
        P("dom", None),
        P("dom"),
        P("dom", None),
        P("dom"),
        P("dom"),
        P("dom", None),
        P("dom"),
        P("dom"),
        P("dom"),
    )
    return jax.shard_map(
        shards, mesh=mesh, in_specs=placed, out_specs=(P("dom"), P()), check_vma=False
    )
```

```python
import functools

import jax
import jax.numpy as jnp
from jax import lax
from jax.experimental import pallas as pl
from jax.experimental.pallas import tpu as pltpu
from jax.sharding import PartitionSpec as P

MESH = pl.DeviceIdType.MESH
HOP = 11
ROWS = 96
LANES = 128
LOADS = 8
SLOTS = 4

R = 4
BLOCK = 128
NEG = 32
FAN1 = 4
FAN2 = 2

HALF, FULL = jnp.bfloat16, jnp.float32


def round_up(value, multiple):
    return (value + multiple - 1) // multiple * multiple


def paired(ref, start, count):
    parts = [ref[pl.ds(start + part, count, stride=2), :] for part in range(2)]
    return jnp.concatenate(parts, axis=1)


def pair_up(ref, start, values):
    count = values.shape[0]
    for part in range(2):
        ref[pl.ds(start + part, count, stride=2), :] = values[:, part * LANES : (part + 1) * LANES]


def greet(devices, me):
    barrier = pltpu.get_barrier_semaphore()

    def hail(step, carry):
        other = lax.rem(me + step, devices)
        pl.semaphore_signal(barrier, inc=1, device_id=(other,), device_id_type=MESH)
        return carry

    lax.fori_loop(1, devices, hail, 0)
    return lambda: pl.semaphore_wait(barrier, devices - 1)


def ranks(devices, owner_ref, blocks):
    lane = lax.broadcasted_iota(jnp.int32, (LANES, 2 * LANES), 1)
    item = lax.broadcasted_iota(jnp.int32, (LANES, 2 * LANES), 0)
    counting = ((item < lane) | (lane >= LANES)).astype(HALF)
    owner_id = lax.broadcasted_iota(jnp.int32, (devices, LANES), 0)
    hots = []
    for block in range(blocks):
        owner = owner_ref[0:1, block * LANES : (block + 1) * LANES]
        hots.append((owner == owner_id).astype(FULL))
    counted = jnp.dot(
        jnp.concatenate(hots, axis=0).astype(HALF), counting, preferred_element_type=FULL
    )
    running = jnp.zeros((devices, LANES), FULL)
    positions = []
    for block in range(blocks):
        mine = counted[block * devices : (block + 1) * devices]
        prior = mine[:, :LANES] + running
        running = running + mine[:, LANES:]
        positions.append(jnp.sum(prior * hots[block], axis=0, keepdims=True))
    return hots, positions


def asked_of(hots, positions, rows, offset, width):
    slot = lax.broadcasted_iota(jnp.int32, (width, LANES), 0).astype(FULL)
    total = None
    for block, (hot, position) in enumerate(zip(hots, positions)):
        row = rows[block]
        high = lax.shift_right_logical(row, 7).astype(FULL)
        low = jnp.bitwise_and(row, 127).astype(FULL)
        digits = jnp.concatenate([hot * high, hot * low], axis=0).astype(HALF)
        placed = (slot == position + float(offset)).astype(FULL).astype(HALF)
        term = lax.dot_general(
            digits, placed, (((1,), (1,)), ((), ())), preferred_element_type=FULL
        )
        total = term if total is None else total + term
    return total


def shares_of(kinds, fan):
    first = lax.broadcasted_iota(jnp.int32, (LANES, LANES), 0) // fan
    second = lax.broadcasted_iota(jnp.int32, (LANES, LANES), 1) // fan
    together = (first == second).astype(HALF)
    count = None
    for kind in range(R):
        same = (kinds == kind).astype(FULL)
        term = same * jnp.dot(same.astype(HALF), together, preferred_element_type=FULL)
        count = term if count is None else count + term
    return 1.0 / jnp.maximum(count, 1.0)


def fetch_kernel(
    devices,
    caps,
    strides,
    counts,
    far_owner,
    first_owner,
    seed_owner,
    far_row,
    first_row,
    seed_row,
    far_kind,
    first_kind,
    features,
    w_first,
    w_second,
    mask,
    loss_out,
    mean_out,
    first_weights,
    second_weights,
    spare_owner,
    spare_row,
    table_half,
    table,
    asks,
    requests,
    arrived,
    wanted,
    look_own,
    look_out,
    look_in,
    share_own,
    share_in,
    look,
    share,
    far_send,
    near_send,
    far_recv,
    near_recv,
    far_cast,
    near_cast,
    staging,
    mine,
    hop_layer,
    seed_input,
    kind_columns,
    piece_send,
    piece_recv,
    second,
    part,
    seen,
    load_sem,
    weight_sem,
    small_sem,
    ask_send,
    ask_recv,
    info_send,
    info_recv,
    far_send_sem,
    far_recv_sem,
    near_send_sem,
    near_recv_sem,
    piece_send_sem,
    piece_recv_sem,
    tell_send,
    tell_recv,
):
    me = lax.axis_index("dom")
    side = devices // 2
    half = lax.div(me, side)
    local = lax.rem(me, side)
    mirror = lax.rem(me + side, devices)
    far_count, first_count, seed_count = counts
    width = features.shape[1]
    far_cap, first_cap, seed_cap = caps
    far_stride, near_stride = strides
    far_rows, near_rows = side * far_stride, side * near_stride
    asked = requests.shape[2]
    nodes = features.shape[0]
    chunk = nodes // LOADS
    loads = [
        pltpu.make_async_copy(
            features.at[pl.ds(turn * chunk, chunk)],
            table_half.at[turn % SLOTS],
            load_sem.at[turn],
        )
        for turn in range(LOADS)
    ]
    for load in loads[:SLOTS]:
        load.start()
    weigh = [
        pltpu.make_async_copy(w_first, first_weights, weight_sem.at[0]),
        pltpu.make_async_copy(w_second, second_weights, weight_sem.at[1]),
    ]
    for copy in weigh:
        copy.start()
    met = greet(devices, me)

    spare_owner[...] = jnp.full(spare_owner.shape, -1, jnp.int32)
    spare_row[...] = jnp.zeros(spare_row.shape, jnp.int32)
    spare_owner[0:1, 0:seed_count] = seed_owner[...]
    spare_row[0:1, 0:seed_count] = seed_row[...]
    far_blocks, first_blocks = far_row.shape[0], first_row.shape[0]
    seed_blocks = spare_row.shape[1] // LANES
    lanes_of = [slice(block * LANES, (block + 1) * LANES) for block in range(far_blocks)]
    far_hot, far_pos = ranks(devices, far_owner, far_blocks)
    first_hot, first_pos = ranks(devices, first_owner, first_blocks)
    seed_hot, seed_pos = ranks(devices, spare_owner, seed_blocks)
    far_rows_of = [far_row[block : block + 1, :] for block in range(far_blocks)]
    first_rows_of = [first_row[block : block + 1, :] for block in range(first_blocks)]
    seed_rows_of = [spare_row[0:1, lanes_of[block]] for block in range(seed_blocks)]
    digits = (
        asked_of(far_hot, far_pos, far_rows_of, 0, asked)
        + asked_of(first_hot, first_pos, first_rows_of, far_stride, asked)
        + asked_of(seed_hot, seed_pos, seed_rows_of, far_stride + first_cap, asked)
    )
    wishes = (digits[:devices] * 128.0 + digits[devices:]).astype(jnp.int32)
    asks[...] = jnp.clip(wishes, 0, nodes - 1) * 2

    def lay(owner, carry):
        requests[owner] = asks[pl.ds(owner, 1), :]
        return carry

    lax.fori_loop(0, devices, lay, 0)
    met()

    def ask(turn, carry):
        other = lax.rem(me + turn * HOP, devices)
        pltpu.make_async_remote_copy(
            src_ref=requests.at[other],
            dst_ref=arrived.at[me],
            send_sem=ask_send,
            recv_sem=ask_recv,
            device_id=(other,),
            device_id_type=MESH,
        ).start()
        return carry

    lax.fori_loop(1, devices, ask, 0)
    own_ask = pltpu.make_async_copy(requests.at[me], arrived.at[me], small_sem.at[0])
    own_ask.start()

    first_base = far_blocks
    turn_base = first_base + first_blocks
    seed_base = turn_base + first_blocks
    looks, shared = seed_base + first_blocks, far_blocks + first_blocks
    seed_lanes = LANES // FAN1
    far_zero, near_zero = R * far_rows, (R + 1) * near_rows

    def place_of(position, cap):
        return jnp.clip(position.astype(jnp.int32), 0, cap - 1)

    def put(owner, place, kind, rows, stride, zero, store):
        for ref, whose in ((look_own, half), (look_out, 1 - half)):
            at = owner - whose * side
            held = (at >= 0) & (at < side)
            index = at * stride + place
            if kind is not None:
                index = index + kind * rows
            store(ref, jnp.where(held, index, zero) * 2)

    def at_row(row):
        def store(ref, value):
            ref[row] = value

        return store

    def at_seeds(block):
        def store(ref, value):
            for turn in range(FAN1):
                row = block * FAN1 + turn
                if row < first_blocks:
                    lanes = slice(turn * seed_lanes, (turn + 1) * seed_lanes)
                    ref[seed_base + row, 0:1, 0:seed_lanes] = value[:, lanes]

        return store

    for block in range(far_blocks):
        owner = far_owner[0:1, lanes_of[block]]
        place = place_of(far_pos[block], far_cap)
        kind = far_kind[block : block + 1, :]
        put(owner, place, kind, far_rows, far_stride, far_zero, at_row(block))
    for block in range(first_blocks):
        owner = first_owner[0:1, lanes_of[block]]
        place = place_of(first_pos[block], first_cap)
        kind = first_kind[block : block + 1, :] + 1
        put(owner, place, None, near_rows, near_stride, near_zero, at_row(first_base + block))
        put(owner, place, kind, near_rows, near_stride, near_zero, at_row(turn_base + block))
    for block in range(seed_blocks):
        owner = spare_owner[0:1, lanes_of[block]]
        place = place_of(seed_pos[block], seed_cap) + first_cap
        put(owner, place, None, near_rows, near_stride, near_zero, at_seeds(block))
    far_share = shares_of(far_kind[...], FAN2)
    first_share = shares_of(first_kind[...], FAN1)
    for block in range(far_blocks):
        share_own[block] = far_share[block : block + 1, :]
    for block in range(first_blocks):
        share_own[far_blocks + block] = first_share[block : block + 1, :]
    tells = []
    for turn, (source, target) in enumerate(((look_out, look_in), (share_own, share_in))):
        tells.append(
            pltpu.make_async_remote_copy(
                src_ref=source,
                dst_ref=target,
                send_sem=info_send.at[turn],
                recv_sem=info_recv.at[turn],
                device_id=(mirror,),
                device_id_type=MESH,
            )
        )
        tells[-1].start()
    keeps = [
        pltpu.make_async_copy(look_own, look.at[pl.ds(0, looks)], small_sem.at[1]),
        pltpu.make_async_copy(share_own, share.at[pl.ds(0, shared)], small_sem.at[2]),
    ]
    for keep in keeps:
        keep.start()

    part_rows = chunk // 4
    for turn in range(LOADS):
        loads[turn].wait()

        def widen(quarter, carry):
            start = pl.multiple_of(quarter * part_rows, part_rows)
            values = table_half[turn % SLOTS, pl.ds(start, part_rows), :].astype(FULL)
            pair_up(table, pl.multiple_of(2 * (turn * chunk + start), 8), values)
            return carry

        lax.fori_loop(0, 4, widen, 0)
        if turn + SLOTS < LOADS:
            loads[turn + SLOTS].start()
    own_ask.wait()
    others = pl.ds(0, devices - 1)
    pltpu.make_async_copy(requests.at[others], arrived.at[others], ask_send).wait()
    pltpu.make_async_copy(requests.at[others], arrived.at[others], ask_recv).wait()
    move = pltpu.make_async_copy(arrived, wanted, small_sem.at[0])
    move.start()
    move.wait()

    def serve(turn):
        whose = lax.rem(half + turn, 2) * side
        parts = (
            (0, far_stride, far_send, far_recv, far_send_sem, far_recv_sem),
            (far_stride, near_stride, near_send, near_recv, near_send_sem, near_recv_sem),
        )

        def one(step, carry):
            relay = lax.rem(local + step * HOP, side)
            client = whose + relay
            for first, stride, send, recv, send_sem, recv_sem in parts:
                for place in range(first, first + stride):
                    row = table[pl.ds(wanted[client, 0, place], 2), :]
                    staging[2 * place : 2 * place + 2, :] = row
                send[client] = paired(staging, 2 * first, stride).astype(HALF)
                where = pl.ds(pl.multiple_of(local * stride, stride), stride)

                @pl.when(step < side)
                def _():
                    pltpu.make_async_remote_copy(
                        src_ref=send.at[client],
                        dst_ref=recv.at[turn, where],
                        send_sem=send_sem.at[turn],
                        recv_sem=recv_sem.at[turn],
                        device_id=(half * side + relay,),
                        device_id_type=MESH,
                    ).start()

                @pl.when(step == side)
                def _():
                    recv[turn, where, :] = send[client]

            return carry

        lax.fori_loop(1, side + 1, one, 0)

    serve(1)
    serve(0)

    far_cast[2 * far_zero : 2 * far_zero + 8, :] = jnp.zeros((8, LANES), FULL)
    near_cast[2 * near_zero : 2 * near_zero + 8, :] = jnp.zeros((8, LANES), FULL)

    lane = lax.broadcasted_iota(jnp.int32, (1, LANES), 1)
    seed_of = lax.broadcasted_iota(jnp.int32, (seed_lanes, LANES), 1) // FAN1
    chosen = (seed_of == lax.broadcasted_iota(jnp.int32, (seed_lanes, LANES), 0)).astype(HALF)
    for block in range(first_blocks):
        kinds = first_kind[block : block + 1, :]
        hot = [
            ((kinds == kind) & (lane % FAN1 == k)).astype(FULL)
            for k in range(FAN1)
            for kind in range(R)
        ]
        kind_columns[block * seed_lanes : (block + 1) * seed_lanes, 0 : FAN1 * R] = lax.dot_general(
            chosen,
            jnp.concatenate(hot, axis=0).astype(HALF),
            (((1,), (1,)), ((), ())),
            preferred_element_type=FULL,
        )

    for copy in weigh:
        copy.wait()
    for tell in tells:
        tell.wait()
    keeps += [
        pltpu.make_async_copy(look_in, look.at[pl.ds(looks, looks)], small_sem.at[3]),
        pltpu.make_async_copy(share_in, share.at[pl.ds(shared, shared)], small_sem.at[4]),
    ]
    for keep in keeps[2:]:
        keep.start()
    for keep in keeps:
        keep.wait()

    def arrive(recv, turn, rows, stride, recv_sem):
        there = pl.ds(0, rows - stride)
        block = recv.at[turn, there]
        pltpu.make_async_copy(block, block, recv_sem.at[turn]).wait()

    def project(recv, turn, rows, cast, first_kind_of, kinds):
        size = rows // 2

        def some(part_of, carry):
            start = pl.multiple_of(part_of * size, size)
            values = recv[turn, pl.ds(start, size), :]
            for kind in range(kinds):
                top = (first_kind_of + kind) * width
                term = jnp.dot(
                    values, first_weights[top : top + width, :], preferred_element_type=FULL
                )
                pair_up(cast, pl.multiple_of(2 * (kind * rows + start), 8), term)
            return carry

        lax.fori_loop(0, 2, some, 0)

    def sums(turn, block, target):
        look_row, share_row = turn * looks, turn * shared

        def at(cast, row, lane_of):
            return cast[pl.ds(look[look_row + row, 0, lane_of], 2), :]

        for item in range(LANES):
            row, first = (item * FAN2) // LANES, (item * FAN2) % LANES
            total = at(far_cast, block * FAN2 + row, first)
            for k in range(1, FAN2):
                total = total + at(far_cast, block * FAN2 + row, first + k)
            scale = share[share_row + block * FAN2 + row, 0, first]
            target[2 * item : 2 * item + 2, :] = (
                at(near_cast, first_base + block, item) + scale * total
            )
        for seed in range(seed_lanes):
            total = at(near_cast, seed_base + block, seed)
            for k in range(FAN1):
                item = seed * FAN1 + k
                scale = share[share_row + far_blocks + block, 0, item]
                total = total + scale * at(near_cast, turn_base + block, item)
            place = 2 * (LANES + seed)
            target[place : place + 2, :] = total

    piece = LANES + seed_lanes
    arrive(far_recv, 1, far_rows, far_stride, far_recv_sem)
    project(far_recv, 1, far_rows, far_cast, 1, R)
    arrive(near_recv, 1, near_rows, near_stride, near_recv_sem)
    project(near_recv, 1, near_rows, near_cast, 0, R + 1)

    def mirror_block(block, carry):
        sums(1, block, staging)
        piece_send[block] = paired(staging, 0, piece).astype(HALF)
        pltpu.make_async_remote_copy(
            src_ref=piece_send.at[block],
            dst_ref=piece_recv.at[block],
            send_sem=piece_send_sem,
            recv_sem=piece_recv_sem,
            device_id=(mirror,),
            device_id_type=MESH,
        ).start()
        return carry

    lax.fori_loop(0, first_blocks, mirror_block, 0)

    arrive(far_recv, 0, far_rows, far_stride, far_recv_sem)
    project(far_recv, 0, far_rows, far_cast, 1, R)
    arrive(near_recv, 0, near_rows, near_stride, near_recv_sem)
    project(near_recv, 0, near_rows, near_cast, 0, R + 1)

    def own_block(block, carry):
        sums(0, block, staging)
        mine[block] = paired(staging, 0, piece)
        return carry

    lax.fori_loop(0, first_blocks, own_block, 0)

    pltpu.make_async_copy(piece_recv, piece_recv, piece_recv_sem).wait()

    def join(block, carry):
        value = jnp.maximum(mine[block] + piece_recv[block].astype(FULL), 0.0).astype(HALF)
        hops = pl.ds(pl.multiple_of(block * LANES, LANES), LANES)
        for part_of in range(2):
            hop_layer[part_of, hops, :] = value[:LANES, lanes_of[part_of]].astype(FULL)
        seeds = pl.ds(pl.multiple_of(block * seed_lanes, seed_lanes), seed_lanes)
        seed_input[seeds, 0:width] = value[LANES:]
        return carry

    lax.fori_loop(0, first_blocks, join, 0)

    def means(turn, carry):
        start = pl.multiple_of(turn * ROWS, ROWS)
        where = pl.ds(start, ROWS)
        values = [
            jnp.concatenate(
                [
                    hop_layer[part_of, pl.ds(start * FAN1 + k, ROWS, stride=FAN1), :]
                    for part_of in range(2)
                ],
                axis=1,
            )
            for k in range(FAN1)
        ]
        columns = kind_columns[where, :]
        for kind in range(R):
            hot = [columns[:, k * R + kind : k * R + kind + 1] for k in range(FAN1)]
            portion = 1.0 / jnp.maximum(sum(hot[1:], hot[0]), 1.0)
            mean = (hot[0] * portion) * values[0]
            for k in range(1, FAN1):
                mean = mean + (hot[k] * portion) * values[k]
            seed_input[where, (kind + 1) * width : (kind + 2) * width] = mean.astype(HALF)
        return carry

    lax.fori_loop(0, seed_count // ROWS, means, 0)
    second[...] = jnp.dot(seed_input[...], second_weights[...], preferred_element_type=FULL)

    blocks = mask.shape[0]
    positives = blocks * BLOCK
    loss_sum = jnp.zeros((1, 1), FULL)
    edge_sum = jnp.zeros((1, 1), FULL)

    diagonal = lax.broadcasted_iota(jnp.int32, (BLOCK, BLOCK), 0) == lax.broadcasted_iota(
        jnp.int32, (BLOCK, BLOCK), 1
    )
    for block in range(blocks):
        sources = second[block * BLOCK : (block + 1) * BLOCK, :]
        targets = second[positives + block * BLOCK : positives + (block + 1) * BLOCK, :]
        first_neg = 2 * positives + block * NEG
        negatives = second[first_neg : first_neg + NEG, :]
        scores = lax.dot_general(
            jnp.concatenate([targets, negatives], axis=0),
            sources,
            (((1,), (1,)), ((), ())),
            precision=lax.Precision.HIGHEST,
            preferred_element_type=FULL,
        )
        positive = jnp.sum(jnp.where(diagonal, scores[:BLOCK], 0.0), axis=0, keepdims=True)
        negative = scores[BLOCK:]
        top_score = jnp.maximum(positive, jnp.max(negative, axis=0, keepdims=True))
        spread_sum = jnp.exp(positive - top_score) + jnp.sum(
            jnp.exp(negative - top_score), axis=0, keepdims=True
        )
        edge_loss = top_score + jnp.log(spread_sum) - positive
        loss_out[block : block + 1, :] = edge_loss
        counted = mask[block : block + 1, :].astype(FULL)
        loss_sum = loss_sum + jnp.sum(counted * edge_loss, axis=1, keepdims=True)
        edge_sum = edge_sum + jnp.sum(counted, axis=1, keepdims=True)
    part[...] = jnp.where(lane == 0, loss_sum, jnp.where(lane == 1, edge_sum, 0.0))

    def tell_all(turn, carry):
        other = lax.rem(me + turn * HOP, devices)
        pltpu.make_async_remote_copy(
            src_ref=part,
            dst_ref=seen.at[me],
            send_sem=tell_send,
            recv_sem=tell_recv,
            device_id=(other,),
            device_id_type=MESH,
        ).start()
        return carry

    lax.fori_loop(1, devices, tell_all, 0)
    seen[me] = part[...]
    near_side = pl.ds(0, side - 1)
    for turn in range(2):
        sent = far_send.at[near_side]
        pltpu.make_async_copy(sent, sent, far_send_sem.at[turn]).wait()
        sent = near_send.at[near_side]
        pltpu.make_async_copy(sent, sent, near_send_sem.at[turn]).wait()
    pltpu.make_async_copy(piece_send, piece_send, piece_send_sem).wait()
    pltpu.make_async_copy(seen.at[others], seen.at[others], tell_recv).wait()
    pltpu.make_async_copy(seen.at[others], seen.at[others], tell_send).wait()
    total = jnp.sum(seen[...], axis=0)
    mean_out[...] = total[:, 0:1] / jnp.maximum(total[:, 1:2], 1.0)


def fetch(owners, rows, kinds, features, w_first, w_second, mask, caps, counts, devices):
    nodes, width = features.shape
    side = devices // 2
    strides = (round_up(caps[0], 16), round_up(caps[1] + caps[2], 16))
    asked = round_up(sum(strides), LANES)
    far_rows, near_rows = side * strides[0], side * strides[1]
    far_blocks, first_blocks = rows[0].shape[0], rows[1].shape[0]
    looks, shared = far_blocks + 3 * first_blocks, far_blocks + first_blocks
    piece = LANES + LANES // FAN1
    number = jnp.int32
    vmem, anywhere = (pl.BlockSpec(memory_space=space) for space in (pltpu.VMEM, pl.ANY))
    return pl.pallas_call(
        functools.partial(fetch_kernel, devices, caps, strides, counts),
        out_shape=[
            jax.ShapeDtypeStruct(mask.shape, FULL),
            jax.ShapeDtypeStruct((1, 1), FULL),
        ],
        in_specs=[vmem] * 8 + [anywhere] * 3 + [vmem],
        out_specs=[vmem, vmem],
        scratch_shapes=[
            pltpu.VMEM(w_first.shape, HALF),
            pltpu.VMEM(w_second.shape, HALF),
            pltpu.VMEM((1, round_up(counts[2], LANES)), number),
            pltpu.VMEM((1, round_up(counts[2], LANES)), number),
            pltpu.VMEM((SLOTS, nodes // LOADS, width), HALF),
            pltpu.VMEM((2 * nodes, LANES), FULL),
            pltpu.VMEM((devices, asked), number),
            pltpu.VMEM((devices, 1, asked), number),
            pltpu.VMEM((devices, 1, asked), number),
            pltpu.SMEM((devices, 1, asked), number),
            pltpu.VMEM((looks, 1, LANES), number),
            pltpu.VMEM((looks, 1, LANES), number),
            pltpu.VMEM((looks, 1, LANES), number),
            pltpu.VMEM((shared, 1, LANES), FULL),
            pltpu.VMEM((shared, 1, LANES), FULL),
            pltpu.SMEM((2 * looks, 1, LANES), number),
            pltpu.SMEM((2 * shared, 1, LANES), FULL),
            pltpu.VMEM((devices, strides[0], width), HALF),
            pltpu.VMEM((devices, strides[1], width), HALF),
            pltpu.VMEM((2, far_rows, width), HALF),
            pltpu.VMEM((2, near_rows, width), HALF),
            pltpu.VMEM((2 * R * far_rows + 8, LANES), FULL),
            pltpu.VMEM((2 * (R + 1) * near_rows + 8, LANES), FULL),
            pltpu.VMEM((2 * max(sum(strides), piece), LANES), FULL),
            pltpu.VMEM((first_blocks, piece, width), FULL),
            pltpu.VMEM((2, counts[1], LANES), FULL),
            pltpu.VMEM((counts[2], (R + 1) * width), HALF),
            pltpu.VMEM((counts[2], LANES), FULL),
            pltpu.VMEM((first_blocks, piece, width), HALF),
            pltpu.VMEM((first_blocks, piece, width), HALF),
            pltpu.VMEM((counts[2], width), FULL),
            pltpu.VMEM((1, LANES), FULL),
            pltpu.VMEM((devices, 1, LANES), FULL),
            pltpu.SemaphoreType.DMA((LOADS,)),
            pltpu.SemaphoreType.DMA((2,)),
            pltpu.SemaphoreType.DMA((5,)),
            pltpu.SemaphoreType.DMA(()),
            pltpu.SemaphoreType.DMA(()),
        ]
        + [pltpu.SemaphoreType.DMA((2,))] * 6
        + [pltpu.SemaphoreType.DMA(())] * 4,
        compiler_params=pltpu.CompilerParams(
            collective_id=0, has_side_effects=True, vmem_limit_bytes=67043328
        ),
        name="fetch",
    )(*owners, *rows, *kinds, features, w_first, w_second, mask)


def shards(
    features,
    w_first,
    w_second,
    seed_owner,
    seed_row,
    hop1_owner,
    hop1_row,
    hop1_rel,
    hop2_owner,
    hop2_row,
    hop2_rel,
    edge_mask,
):
    devices = lax.axis_size("dom")
    counts = (hop2_row.shape[0], hop1_row.shape[0], seed_row.shape[0])
    caps = tuple((2 * length + devices - 1) // devices for length in counts)

    owners = [owner.reshape(1, -1) for owner in (hop2_owner, hop1_owner, seed_owner)]
    rows = [hop2_row.reshape(-1, LANES), hop1_row.reshape(-1, LANES), seed_row.reshape(1, -1)]
    edge_loss, mean_loss = fetch(
        owners,
        rows,
        [rel.reshape(-1, LANES) for rel in (hop2_rel, hop1_rel)],
        features,
        w_first,
        w_second,
        edge_mask.reshape(-1, BLOCK),
        caps,
        counts,
        devices,
    )
    return (edge_loss.reshape(-1), mean_loss[0, 0])


def solution(mesh):
    placed = (
        P("dom", None),
        P(),
        P(),
        P("dom", None),
        P("dom"),
        P("dom", None),
        P("dom"),
        P("dom"),
        P("dom", None),
        P("dom"),
        P("dom"),
        P("dom"),
    )
    return jax.shard_map(
        shards, mesh=mesh, in_specs=placed, out_specs=(P("dom"), P()), check_vma=False
    )
```

```python
import functools

import jax
import jax.numpy as jnp
from jax import lax
from jax.experimental import pallas as pl
from jax.experimental.pallas import tpu as pltpu
from jax.sharding import PartitionSpec as P

MESH = pl.DeviceIdType.MESH
HOP = 11
LANES = 128
LOADS = 8
SLOTS = 4

R = 4
BLOCK = 128
NEG = 32
FAN1 = 4
FAN2 = 2

HALF, FULL = jnp.bfloat16, jnp.float32


def round_up(value, multiple):
    return (value + multiple - 1) // multiple * multiple


def paired(ref, start, count):
    parts = [ref[pl.ds(start + part, count, stride=2), :] for part in range(2)]
    return jnp.concatenate(parts, axis=1)


def pair_up(ref, start, values):
    count = values.shape[0]
    for part in range(2):
        ref[pl.ds(start + part, count, stride=2), :] = values[:, part * LANES : (part + 1) * LANES]


def greet(devices, me):
    barrier = pltpu.get_barrier_semaphore()

    def hail(step, carry):
        other = lax.rem(me + step, devices)
        pl.semaphore_signal(barrier, inc=1, device_id=(other,), device_id_type=MESH)
        return carry

    lax.fori_loop(1, devices, hail, 0)
    return lambda: pl.semaphore_wait(barrier, devices - 1)


def ranks(devices, owner_ref, blocks):
    lane = lax.broadcasted_iota(jnp.int32, (LANES, 2 * LANES), 1)
    item = lax.broadcasted_iota(jnp.int32, (LANES, 2 * LANES), 0)
    counting = ((item < lane) | (lane >= LANES)).astype(HALF)
    owner_id = lax.broadcasted_iota(jnp.int32, (devices, LANES), 0)
    hots = []
    for block in range(blocks):
        owner = owner_ref[0:1, block * LANES : (block + 1) * LANES]
        hots.append((owner == owner_id).astype(FULL))
    counted = jnp.dot(
        jnp.concatenate(hots, axis=0).astype(HALF), counting, preferred_element_type=FULL
    )
    running = jnp.zeros((devices, LANES), FULL)
    positions = []
    for block in range(blocks):
        mine = counted[block * devices : (block + 1) * devices]
        prior = mine[:, :LANES] + running
        running = running + mine[:, LANES:]
        positions.append(jnp.sum(prior * hots[block], axis=0, keepdims=True))
    return hots, positions


def asked_of(hots, positions, rows, offset, width):
    slot = lax.broadcasted_iota(jnp.int32, (width, LANES), 0).astype(FULL)
    total = None
    for block, (hot, position) in enumerate(zip(hots, positions)):
        row = rows[block]
        high = lax.shift_right_logical(row, 7).astype(FULL)
        low = jnp.bitwise_and(row, 127).astype(FULL)
        digits = jnp.concatenate([hot * high, hot * low], axis=0).astype(HALF)
        placed = (slot == position + float(offset)).astype(FULL).astype(HALF)
        term = lax.dot_general(
            digits, placed, (((1,), (1,)), ((), ())), preferred_element_type=FULL
        )
        total = term if total is None else total + term
    return total


def shares_of(kinds, fan):
    first = lax.broadcasted_iota(jnp.int32, (LANES, LANES), 0) // fan
    second = lax.broadcasted_iota(jnp.int32, (LANES, LANES), 1) // fan
    together = (first == second).astype(HALF)
    count = None
    for kind in range(R):
        same = (kinds == kind).astype(FULL)
        term = same * jnp.dot(same.astype(HALF), together, preferred_element_type=FULL)
        count = term if count is None else count + term
    return 1.0 / jnp.maximum(count, 1.0)


def fetch_kernel(
    devices,
    caps,
    strides,
    counts,
    far_owner,
    first_owner,
    seed_owner,
    far_row,
    first_row,
    seed_row,
    far_kind,
    first_kind,
    features,
    w_first,
    w_second,
    mask,
    loss_out,
    mean_out,
    first_weights,
    second_weights,
    spare_owner,
    spare_row,
    table_half,
    table,
    asks,
    requests,
    arrived,
    wanted,
    look_own,
    look_out,
    look_in,
    share_own,
    share_in,
    look,
    share,
    far_send,
    near_send,
    far_recv,
    near_recv,
    far_cast,
    near_cast,
    staging,
    mine,
    hop_layer,
    kind_columns,
    piece_send,
    piece_recv,
    second,
    part,
    seen,
    load_sem,
    weight_sem,
    small_sem,
    ask_send,
    ask_recv,
    info_send,
    info_recv,
    far_send_sem,
    far_recv_sem,
    near_send_sem,
    near_recv_sem,
    piece_send_sem,
    piece_recv_sem,
    tell_send,
    tell_recv,
):
    me = lax.axis_index("dom")
    side = devices // 2
    half = lax.div(me, side)
    local = lax.rem(me, side)
    mirror = lax.rem(me + side, devices)
    far_count, first_count, seed_count = counts
    width = features.shape[1]
    far_cap, first_cap, seed_cap = caps
    far_stride, near_stride = strides
    far_rows, near_rows = side * far_stride, side * near_stride
    asked = requests.shape[2]
    nodes = features.shape[0]
    chunk = nodes // LOADS
    loads = [
        pltpu.make_async_copy(
            features.at[pl.ds(turn * chunk, chunk)],
            table_half.at[turn % SLOTS],
            load_sem.at[turn],
        )
        for turn in range(LOADS)
    ]
    for load in loads[:SLOTS]:
        load.start()
    weigh = [
        pltpu.make_async_copy(w_first, first_weights, weight_sem.at[0]),
        pltpu.make_async_copy(w_second, second_weights, weight_sem.at[1]),
    ]
    for copy in weigh:
        copy.start()
    met = greet(devices, me)

    spare_owner[...] = jnp.full(spare_owner.shape, -1, jnp.int32)
    spare_row[...] = jnp.zeros(spare_row.shape, jnp.int32)
    spare_owner[0:1, 0:seed_count] = seed_owner[...]
    spare_row[0:1, 0:seed_count] = seed_row[...].reshape(1, seed_count)
    far_blocks, first_blocks = far_row.shape[0], first_row.shape[0]
    seed_blocks = spare_row.shape[1] // LANES
    lanes_of = [slice(block * LANES, (block + 1) * LANES) for block in range(far_blocks)]
    far_hot, far_pos = ranks(devices, far_owner, far_blocks)
    first_hot, first_pos = ranks(devices, first_owner, first_blocks)
    seed_hot, seed_pos = ranks(devices, spare_owner, seed_blocks)
    far_rows_of = [far_row[block : block + 1, :] for block in range(far_blocks)]
    first_rows_of = [first_row[block : block + 1, :] for block in range(first_blocks)]
    seed_rows_of = [spare_row[0:1, lanes_of[block]] for block in range(seed_blocks)]
    digits = (
        asked_of(far_hot, far_pos, far_rows_of, 0, asked)
        + asked_of(first_hot, first_pos, first_rows_of, far_stride, asked)
        + asked_of(seed_hot, seed_pos, seed_rows_of, far_stride + first_cap, asked)
    )
    wishes = (digits[:devices] * 128.0 + digits[devices:]).astype(jnp.int32)
    asks[...] = jnp.clip(wishes, 0, nodes - 1) * 2

    def lay(owner, carry):
        requests[owner] = asks[pl.ds(owner, 1), :]
        return carry

    lax.fori_loop(0, devices, lay, 0)
    met()

    def ask(turn, carry):
        other = lax.rem(me + turn * HOP, devices)
        pltpu.make_async_remote_copy(
            src_ref=requests.at[other],
            dst_ref=arrived.at[me],
            send_sem=ask_send,
            recv_sem=ask_recv,
            device_id=(other,),
            device_id_type=MESH,
        ).start()
        return carry

    lax.fori_loop(1, devices, ask, 0)
    own_ask = pltpu.make_async_copy(requests.at[me], arrived.at[me], small_sem.at[0])
    own_ask.start()

    first_base = far_blocks
    turn_base = first_base + first_blocks
    seed_base = turn_base + first_blocks
    looks, shared = seed_base + first_blocks, far_blocks + first_blocks
    seed_lanes = LANES // FAN1
    far_zero, near_zero = R * far_rows, (R + 1) * near_rows

    def place_of(position, cap):
        return jnp.clip(position.astype(jnp.int32), 0, cap - 1)

    def put(owner, place, kind, rows, stride, zero, store):
        for ref, whose in ((look_own, half), (look_out, 1 - half)):
            at = owner - whose * side
            held = (at >= 0) & (at < side)
            index = at * stride + place
            if kind is not None:
                index = index + kind * rows
            store(ref, jnp.where(held, index, zero) * 2)

    def at_row(row):
        def store(ref, value):
            ref[row] = value

        return store

    def at_seeds(block):
        def store(ref, value):
            for turn in range(FAN1):
                row = block * FAN1 + turn
                if row < first_blocks:
                    lanes = slice(turn * seed_lanes, (turn + 1) * seed_lanes)
                    ref[seed_base + row, 0:1, 0:seed_lanes] = value[:, lanes]

        return store

    for block in range(far_blocks):
        owner = far_owner[0:1, lanes_of[block]]
        place = place_of(far_pos[block], far_cap)
        kind = far_kind[block : block + 1, :]
        put(owner, place, kind, far_rows, far_stride, far_zero, at_row(block))
    for block in range(first_blocks):
        owner = first_owner[0:1, lanes_of[block]]
        place = place_of(first_pos[block], first_cap)
        kind = first_kind[block : block + 1, :] + 1
        put(owner, place, None, near_rows, near_stride, near_zero, at_row(first_base + block))
        put(owner, place, kind, near_rows, near_stride, near_zero, at_row(turn_base + block))
    for block in range(seed_blocks):
        owner = spare_owner[0:1, lanes_of[block]]
        place = place_of(seed_pos[block], seed_cap) + first_cap
        put(owner, place, None, near_rows, near_stride, near_zero, at_seeds(block))
    far_share = shares_of(far_kind[...], FAN2)
    first_share = shares_of(first_kind[...], FAN1)
    for block in range(far_blocks):
        share_own[block] = far_share[block : block + 1, :]
    for block in range(first_blocks):
        share_own[far_blocks + block] = first_share[block : block + 1, :]
    tells = []
    for turn, (source, target) in enumerate(((look_out, look_in), (share_own, share_in))):
        tells.append(
            pltpu.make_async_remote_copy(
                src_ref=source,
                dst_ref=target,
                send_sem=info_send.at[turn],
                recv_sem=info_recv.at[turn],
                device_id=(mirror,),
                device_id_type=MESH,
            )
        )
        tells[-1].start()
    keeps = [
        pltpu.make_async_copy(look_own, look.at[pl.ds(0, looks)], small_sem.at[1]),
        pltpu.make_async_copy(share_own, share.at[pl.ds(0, shared)], small_sem.at[2]),
    ]
    for keep in keeps:
        keep.start()

    part_rows = chunk // 4
    for turn in range(LOADS):
        loads[turn].wait()

        def widen(quarter, carry):
            start = pl.multiple_of(quarter * part_rows, part_rows)
            values = table_half[turn % SLOTS, pl.ds(start, part_rows), :].astype(FULL)
            pair_up(table, pl.multiple_of(2 * (turn * chunk + start), 8), values)
            return carry

        lax.fori_loop(0, 4, widen, 0)
        if turn + SLOTS < LOADS:
            loads[turn + SLOTS].start()
    own_ask.wait()
    others = pl.ds(0, devices - 1)
    pltpu.make_async_copy(requests.at[others], arrived.at[others], ask_send).wait()
    pltpu.make_async_copy(requests.at[others], arrived.at[others], ask_recv).wait()
    moves = []
    for turn in range(2):
        clients = pl.ds(lax.rem(half + turn, 2) * side, side)
        moves.append(
            pltpu.make_async_copy(arrived.at[clients], wanted.at[clients], small_sem.at[5 + turn])
        )
    moves[1].start()
    moves[0].start()
    moves[1].wait()

    def serve(turn):
        whose = lax.rem(half + turn, 2) * side
        parts = (
            (0, far_stride, far_send, far_recv, far_send_sem, far_recv_sem),
            (far_stride, near_stride, near_send, near_recv, near_send_sem, near_recv_sem),
        )

        def one(step, carry):
            relay = lax.rem(local + step * HOP, side)
            client = whose + relay
            for first, stride, send, recv, send_sem, recv_sem in parts:
                for place in range(first, first + stride):
                    row = table[pl.ds(wanted[client, 0, place], 2), :]
                    staging[2 * place : 2 * place + 2, :] = row
                send[client] = paired(staging, 2 * first, stride).astype(HALF)
                where = pl.ds(pl.multiple_of(local * stride, stride), stride)

                @pl.when(step < side)
                def _():
                    pltpu.make_async_remote_copy(
                        src_ref=send.at[client],
                        dst_ref=recv.at[turn, where],
                        send_sem=send_sem.at[turn],
                        recv_sem=recv_sem.at[turn],
                        device_id=(half * side + relay,),
                        device_id_type=MESH,
                    ).start()

                @pl.when(step == side)
                def _():
                    recv[turn, where, :] = send[client]

            return carry

        lax.fori_loop(1, side + 1, one, 0)

    serve(1)
    moves[0].wait()
    serve(0)

    far_cast[2 * far_zero : 2 * far_zero + 8, :] = jnp.zeros((8, LANES), FULL)
    near_cast[2 * near_zero : 2 * near_zero + 8, :] = jnp.zeros((8, LANES), FULL)

    lane = lax.broadcasted_iota(jnp.int32, (1, LANES), 1)
    seed_of = lax.broadcasted_iota(jnp.int32, (seed_lanes, LANES), 1) // FAN1
    chosen = (seed_of == lax.broadcasted_iota(jnp.int32, (seed_lanes, LANES), 0)).astype(HALF)
    for block in range(first_blocks):
        kinds = first_kind[block : block + 1, :]
        hot = [
            ((kinds == kind) & (lane % FAN1 == k)).astype(FULL)
            for k in range(FAN1)
            for kind in range(R)
        ]
        kind_columns[block * seed_lanes : (block + 1) * seed_lanes, 0 : FAN1 * R] = lax.dot_general(
            chosen,
            jnp.concatenate(hot, axis=0).astype(HALF),
            (((1,), (1,)), ((), ())),
            preferred_element_type=FULL,
        )

    for copy in weigh:
        copy.wait()
    for tell in tells:
        tell.wait()
    keeps += [
        pltpu.make_async_copy(look_in, look.at[pl.ds(looks, looks)], small_sem.at[3]),
        pltpu.make_async_copy(share_in, share.at[pl.ds(shared, shared)], small_sem.at[4]),
    ]
    for keep in keeps[2:]:
        keep.start()
    for keep in keeps:
        keep.wait()

    def arrive(recv, turn, rows, stride, recv_sem):
        there = pl.ds(0, rows - stride)
        block = recv.at[turn, there]
        pltpu.make_async_copy(block, block, recv_sem.at[turn]).wait()

    def project(recv, turn, rows, cast, first_kind_of, kinds):
        size = rows // 2

        def some(part_of, carry):
            start = pl.multiple_of(part_of * size, size)
            values = recv[turn, pl.ds(start, size), :]
            for kind in range(kinds):
                top = (first_kind_of + kind) * width
                term = jnp.dot(
                    values, first_weights[top : top + width, :], preferred_element_type=FULL
                )
                pair_up(cast, pl.multiple_of(2 * (kind * rows + start), 8), term)
            return carry

        lax.fori_loop(0, 2, some, 0)

    def sums(turn, block, target):
        look_row, share_row = turn * looks, turn * shared

        def at(cast, row, lane_of):
            return cast[pl.ds(look[look_row + row, 0, lane_of], 2), :]

        for item in range(LANES):
            row, first = (item * FAN2) // LANES, (item * FAN2) % LANES
            total = at(far_cast, block * FAN2 + row, first)
            for k in range(1, FAN2):
                total = total + at(far_cast, block * FAN2 + row, first + k)
            scale = share[share_row + block * FAN2 + row, 0, first]
            target[2 * item : 2 * item + 2, :] = (
                at(near_cast, first_base + block, item) + scale * total
            )
        for seed in range(seed_lanes):
            total = at(near_cast, seed_base + block, seed)
            for k in range(FAN1):
                item = seed * FAN1 + k
                scale = share[share_row + far_blocks + block, 0, item]
                total = total + scale * at(near_cast, turn_base + block, item)
            place = 2 * (LANES + seed)
            target[place : place + 2, :] = total

    piece = LANES + seed_lanes
    arrive(far_recv, 1, far_rows, far_stride, far_recv_sem)
    project(far_recv, 1, far_rows, far_cast, 1, R)
    arrive(near_recv, 1, near_rows, near_stride, near_recv_sem)
    project(near_recv, 1, near_rows, near_cast, 0, R + 1)

    def mirror_block(block, carry):
        sums(1, block, staging)
        piece_send[block] = paired(staging, 0, piece).astype(HALF)
        pltpu.make_async_remote_copy(
            src_ref=piece_send.at[block],
            dst_ref=piece_recv.at[block],
            send_sem=piece_send_sem,
            recv_sem=piece_recv_sem.at[block],
            device_id=(mirror,),
            device_id_type=MESH,
        ).start()
        return carry

    lax.fori_loop(0, first_blocks, mirror_block, 0)

    arrive(far_recv, 0, far_rows, far_stride, far_recv_sem)
    project(far_recv, 0, far_rows, far_cast, 1, R)
    arrive(near_recv, 0, near_rows, near_stride, near_recv_sem)
    project(near_recv, 0, near_rows, near_cast, 0, R + 1)

    def own_block(block, carry):
        sums(0, block, staging)
        mine[block] = paired(staging, 0, piece)
        return carry

    lax.fori_loop(0, first_blocks, own_block, 0)

    def join(block, carry):
        pltpu.make_async_copy(
            piece_recv.at[block], piece_recv.at[block], piece_recv_sem.at[block]
        ).wait()
        value = jnp.maximum(mine[block] + piece_recv[block].astype(FULL), 0.0).astype(HALF)
        for part_of in range(2):
            hop_layer[part_of] = value[:LANES, lanes_of[part_of]].astype(FULL)
        values = [
            jnp.concatenate(
                [hop_layer[part_of, pl.ds(k, seed_lanes, stride=FAN1), :] for part_of in range(2)],
                axis=1,
            )
            for k in range(FAN1)
        ]
        seeds = pl.ds(pl.multiple_of(block * seed_lanes, seed_lanes), seed_lanes)
        columns = kind_columns[seeds, :]
        inputs = [value[LANES:]]
        for kind in range(R):
            hot = [columns[:, k * R + kind : k * R + kind + 1] for k in range(FAN1)]
            portion = 1.0 / jnp.maximum(sum(hot[1:], hot[0]), 1.0)
            mean = (hot[0] * portion) * values[0]
            for k in range(1, FAN1):
                mean = mean + (hot[k] * portion) * values[k]
            inputs.append(mean.astype(HALF))
        second[seeds, :] = jnp.dot(
            jnp.concatenate(inputs, axis=1), second_weights[...], preferred_element_type=FULL
        )
        return carry

    lax.fori_loop(0, first_blocks, join, 0)

    blocks = mask.shape[0]
    positives = blocks * BLOCK
    loss_sum = jnp.zeros((1, 1), FULL)
    edge_sum = jnp.zeros((1, 1), FULL)

    diagonal = lax.broadcasted_iota(jnp.int32, (BLOCK, BLOCK), 0) == lax.broadcasted_iota(
        jnp.int32, (BLOCK, BLOCK), 1
    )
    for block in range(blocks):
        sources = second[block * BLOCK : (block + 1) * BLOCK, :]
        targets = second[positives + block * BLOCK : positives + (block + 1) * BLOCK, :]
        first_neg = 2 * positives + block * NEG
        negatives = second[first_neg : first_neg + NEG, :]
        scores = lax.dot_general(
            jnp.concatenate([targets, negatives], axis=0),
            sources,
            (((1,), (1,)), ((), ())),
            precision=lax.Precision.HIGHEST,
            preferred_element_type=FULL,
        )
        positive = jnp.sum(jnp.where(diagonal, scores[:BLOCK], 0.0), axis=0, keepdims=True)
        negative = scores[BLOCK:]
        top_score = jnp.maximum(positive, jnp.max(negative, axis=0, keepdims=True))
        spread_sum = jnp.exp(positive - top_score) + jnp.sum(
            jnp.exp(negative - top_score), axis=0, keepdims=True
        )
        edge_loss = top_score + jnp.log(spread_sum) - positive
        loss_out[block : block + 1, :] = edge_loss
        counted = mask[block : block + 1, :].astype(FULL)
        loss_sum = loss_sum + jnp.sum(counted * edge_loss, axis=1, keepdims=True)
        edge_sum = edge_sum + jnp.sum(counted, axis=1, keepdims=True)
    part[...] = jnp.where(lane == 0, loss_sum, jnp.where(lane == 1, edge_sum, 0.0))

    def tell_all(turn, carry):
        other = lax.rem(me + turn * HOP, devices)
        pltpu.make_async_remote_copy(
            src_ref=part,
            dst_ref=seen.at[me],
            send_sem=tell_send,
            recv_sem=tell_recv,
            device_id=(other,),
            device_id_type=MESH,
        ).start()
        return carry

    lax.fori_loop(1, devices, tell_all, 0)
    seen[me] = part[...]
    near_side = pl.ds(0, side - 1)
    for turn in range(2):
        sent = far_send.at[near_side]
        pltpu.make_async_copy(sent, sent, far_send_sem.at[turn]).wait()
        sent = near_send.at[near_side]
        pltpu.make_async_copy(sent, sent, near_send_sem.at[turn]).wait()
    pltpu.make_async_copy(piece_send, piece_send, piece_send_sem).wait()
    pltpu.make_async_copy(seen.at[others], seen.at[others], tell_recv).wait()
    pltpu.make_async_copy(seen.at[others], seen.at[others], tell_send).wait()
    total = jnp.sum(seen[...], axis=0)
    mean_out[...] = total[:, 0:1] / jnp.maximum(total[:, 1:2], 1.0)


def fetch(owners, rows, kinds, features, w_first, w_second, mask, caps, counts, devices):
    nodes, width = features.shape
    side = devices // 2
    strides = (round_up(caps[0], 16), round_up(caps[1] + caps[2], 16))
    asked = round_up(sum(strides), LANES)
    far_rows, near_rows = side * strides[0], side * strides[1]
    far_blocks, first_blocks = rows[0].shape[0], rows[1].shape[0]
    looks, shared = far_blocks + 3 * first_blocks, far_blocks + first_blocks
    piece = LANES + LANES // FAN1
    number = jnp.int32
    vmem, anywhere = (pl.BlockSpec(memory_space=space) for space in (pltpu.VMEM, pl.ANY))
    return pl.pallas_call(
        functools.partial(fetch_kernel, devices, caps, strides, counts),
        out_shape=[
            jax.ShapeDtypeStruct(mask.shape, FULL),
            jax.ShapeDtypeStruct((1, 1), FULL),
        ],
        in_specs=[vmem] * 8 + [anywhere] * 3 + [vmem],
        out_specs=[vmem, vmem],
        scratch_shapes=[
            pltpu.VMEM(w_first.shape, HALF),
            pltpu.VMEM(w_second.shape, HALF),
            pltpu.VMEM((1, round_up(counts[2], LANES)), number),
            pltpu.VMEM((1, round_up(counts[2], LANES)), number),
            pltpu.VMEM((SLOTS, nodes // LOADS, width), HALF),
            pltpu.VMEM((2 * nodes, LANES), FULL),
            pltpu.VMEM((devices, asked), number),
            pltpu.VMEM((devices, 1, asked), number),
            pltpu.VMEM((devices, 1, asked), number),
            pltpu.SMEM((devices, 1, asked), number),
            pltpu.VMEM((looks, 1, LANES), number),
            pltpu.VMEM((looks, 1, LANES), number),
            pltpu.VMEM((looks, 1, LANES), number),
            pltpu.VMEM((shared, 1, LANES), FULL),
            pltpu.VMEM((shared, 1, LANES), FULL),
            pltpu.SMEM((2 * looks, 1, LANES), number),
            pltpu.SMEM((2 * shared, 1, LANES), FULL),
            pltpu.VMEM((devices, strides[0], width), HALF),
            pltpu.VMEM((devices, strides[1], width), HALF),
            pltpu.VMEM((2, far_rows, width), HALF),
            pltpu.VMEM((2, near_rows, width), HALF),
            pltpu.VMEM((2 * R * far_rows + 8, LANES), FULL),
            pltpu.VMEM((2 * (R + 1) * near_rows + 8, LANES), FULL),
            pltpu.VMEM((2 * max(sum(strides), piece), LANES), FULL),
            pltpu.VMEM((first_blocks, piece, width), FULL),
            pltpu.VMEM((2, LANES, LANES), FULL),
            pltpu.VMEM((counts[2], LANES), FULL),
            pltpu.VMEM((first_blocks, piece, width), HALF),
            pltpu.VMEM((first_blocks, piece, width), HALF),
            pltpu.VMEM((counts[2], width), FULL),
            pltpu.VMEM((1, LANES), FULL),
            pltpu.VMEM((devices, 1, LANES), FULL),
            pltpu.SemaphoreType.DMA((LOADS,)),
            pltpu.SemaphoreType.DMA((2,)),
            pltpu.SemaphoreType.DMA((7,)),
            pltpu.SemaphoreType.DMA(()),
            pltpu.SemaphoreType.DMA(()),
        ]
        + [pltpu.SemaphoreType.DMA((2,))] * 6
        + [pltpu.SemaphoreType.DMA(())]
        + [pltpu.SemaphoreType.DMA((first_blocks,))]
        + [pltpu.SemaphoreType.DMA(())] * 2,
        compiler_params=pltpu.CompilerParams(
            collective_id=0, has_side_effects=True, vmem_limit_bytes=67043328
        ),
        name="fetch",
    )(*owners, *rows, *kinds, features, w_first, w_second, mask)


def shards(
    features,
    w_first,
    w_second,
    seed_owner,
    seed_row,
    hop1_owner,
    hop1_row,
    hop1_rel,
    hop2_owner,
    hop2_row,
    hop2_rel,
    edge_mask,
):
    devices = lax.axis_size("dom")
    counts = (hop2_row.shape[0], hop1_row.shape[0], seed_row.shape[0])
    caps = tuple((2 * length + devices - 1) // devices for length in counts)

    owners = [owner.reshape(1, -1) for owner in (hop2_owner, hop1_owner, seed_owner)]
    rows = [hop2_row.reshape(-1, LANES), hop1_row.reshape(-1, LANES), seed_row]
    edge_loss, mean_loss = fetch(
        owners,
        rows,
        [rel.reshape(-1, LANES) for rel in (hop2_rel, hop1_rel)],
        features,
        w_first,
        w_second,
        edge_mask.reshape(-1, BLOCK),
        caps,
        counts,
        devices,
    )
    return (edge_loss.reshape(-1), mean_loss[0, 0])


def solution(mesh):
    placed = (
        P("dom", None),
        P(),
        P(),
        P("dom", None),
        P("dom"),
        P("dom", None),
        P("dom"),
        P("dom"),
        P("dom", None),
        P("dom"),
        P("dom"),
        P("dom"),
    )
    return jax.shard_map(
        shards, mesh=mesh, in_specs=placed, out_specs=(P("dom"), P()), check_vma=False
    )
```

```python
import functools

import jax
import jax.numpy as jnp
from jax import lax
from jax.experimental import pallas as pl
from jax.experimental.pallas import tpu as pltpu
from jax.sharding import PartitionSpec as P

MESH = pl.DeviceIdType.MESH
HOP = 11
LANES = 128
LOADS = 8
SLOTS = 4

R = 4
BLOCK = 128
NEG = 32
FAN1 = 4
FAN2 = 2

HALF, FULL = jnp.bfloat16, jnp.float32


def round_up(value, multiple):
    return (value + multiple - 1) // multiple * multiple


def paired(ref, start, count):
    parts = [ref[pl.ds(start + part, count, stride=2), :] for part in range(2)]
    return jnp.concatenate(parts, axis=1)


def pair_up(ref, start, values):
    count = values.shape[0]
    for part in range(2):
        ref[pl.ds(start + part, count, stride=2), :] = values[:, part * LANES : (part + 1) * LANES]


def greet(devices, me):
    barrier = pltpu.get_barrier_semaphore()

    def hail(step, carry):
        other = lax.rem(me + step, devices)
        pl.semaphore_signal(barrier, inc=1, device_id=(other,), device_id_type=MESH)
        return carry

    lax.fori_loop(1, devices, hail, 0)
    return lambda: pl.semaphore_wait(barrier, devices - 1)


def ranks(devices, owner_ref, blocks):
    lane = lax.broadcasted_iota(jnp.int32, (LANES, 2 * LANES), 1)
    item = lax.broadcasted_iota(jnp.int32, (LANES, 2 * LANES), 0)
    counting = ((item < lane) | (lane >= LANES)).astype(HALF)
    owner_id = lax.broadcasted_iota(jnp.int32, (devices, LANES), 0)
    hots = []
    for block in range(blocks):
        owner = owner_ref[0:1, block * LANES : (block + 1) * LANES]
        hots.append((owner == owner_id).astype(FULL))
    counted = jnp.dot(
        jnp.concatenate(hots, axis=0).astype(HALF), counting, preferred_element_type=FULL
    )
    running = jnp.zeros((devices, LANES), FULL)
    positions = []
    for block in range(blocks):
        mine = counted[block * devices : (block + 1) * devices]
        prior = mine[:, :LANES] + running
        running = running + mine[:, LANES:]
        positions.append(jnp.sum(prior * hots[block], axis=0, keepdims=True))
    return hots, positions


def asked_of(hots, positions, rows, offset, width):
    slot = lax.broadcasted_iota(jnp.int32, (width, LANES), 0).astype(FULL)
    total = None
    for block, (hot, position) in enumerate(zip(hots, positions)):
        row = rows[block]
        high = lax.shift_right_logical(row, 7).astype(FULL)
        low = jnp.bitwise_and(row, 127).astype(FULL)
        digits = jnp.concatenate([hot * high, hot * low], axis=0).astype(HALF)
        placed = (slot == position + float(offset)).astype(FULL).astype(HALF)
        term = lax.dot_general(
            digits, placed, (((1,), (1,)), ((), ())), preferred_element_type=FULL
        )
        total = term if total is None else total + term
    return total


def shares_of(kinds, fan):
    first = lax.broadcasted_iota(jnp.int32, (LANES, LANES), 0) // fan
    second = lax.broadcasted_iota(jnp.int32, (LANES, LANES), 1) // fan
    together = (first == second).astype(HALF)
    count = None
    for kind in range(R):
        same = (kinds == kind).astype(FULL)
        term = same * jnp.dot(same.astype(HALF), together, preferred_element_type=FULL)
        count = term if count is None else count + term
    return 1.0 / jnp.maximum(count, 1.0)


def fetch_kernel(
    devices,
    caps,
    strides,
    counts,
    far_owner,
    first_owner,
    seed_owner,
    far_row,
    first_row,
    seed_row,
    far_kind,
    first_kind,
    features,
    w_first,
    w_second,
    mask,
    loss_out,
    mean_out,
    first_weights,
    second_weights,
    spare_owner,
    spare_row,
    table_half,
    table,
    asks,
    requests,
    arrived,
    wanted,
    look_own,
    look_out,
    look_in,
    share_own,
    share_in,
    look,
    share,
    far_send,
    near_send,
    far_recv,
    near_recv,
    far_cast,
    near_cast,
    staging,
    far_total,
    mine,
    hop_layer,
    kind_columns,
    piece_send,
    piece_recv,
    second,
    part,
    seen,
    load_sem,
    weight_sem,
    small_sem,
    ask_send,
    ask_recv,
    info_send,
    info_recv,
    far_send_sem,
    far_recv_sem,
    near_send_sem,
    near_recv_sem,
    piece_send_sem,
    piece_recv_sem,
    tell_send,
    tell_recv,
):
    me = lax.axis_index("dom")
    side = devices // 2
    half = lax.div(me, side)
    local = lax.rem(me, side)
    mirror = lax.rem(me + side, devices)
    far_count, first_count, seed_count = counts
    width = features.shape[1]
    far_cap, first_cap, seed_cap = caps
    far_stride, near_stride = strides
    far_rows, near_rows = side * far_stride, side * near_stride
    asked = requests.shape[2]
    nodes = features.shape[0]
    chunk = nodes // LOADS
    loads = [
        pltpu.make_async_copy(
            features.at[pl.ds(turn * chunk, chunk)],
            table_half.at[turn % SLOTS],
            load_sem.at[turn],
        )
        for turn in range(LOADS)
    ]
    for load in loads[:SLOTS]:
        load.start()
    weigh = [
        pltpu.make_async_copy(w_first, first_weights, weight_sem.at[0]),
        pltpu.make_async_copy(w_second, second_weights, weight_sem.at[1]),
    ]
    for copy in weigh:
        copy.start()
    met = greet(devices, me)

    spare_owner[...] = jnp.full(spare_owner.shape, -1, jnp.int32)
    spare_row[...] = jnp.zeros(spare_row.shape, jnp.int32)
    spare_owner[0:1, 0:seed_count] = seed_owner[...]
    spare_row[0:1, 0:seed_count] = seed_row[...].reshape(1, seed_count)
    far_blocks, first_blocks = far_row.shape[0], first_row.shape[0]
    seed_blocks = spare_row.shape[1] // LANES
    lanes_of = [slice(block * LANES, (block + 1) * LANES) for block in range(far_blocks)]
    far_hot, far_pos = ranks(devices, far_owner, far_blocks)
    first_hot, first_pos = ranks(devices, first_owner, first_blocks)
    seed_hot, seed_pos = ranks(devices, spare_owner, seed_blocks)
    far_rows_of = [far_row[block : block + 1, :] for block in range(far_blocks)]
    first_rows_of = [first_row[block : block + 1, :] for block in range(first_blocks)]
    seed_rows_of = [spare_row[0:1, lanes_of[block]] for block in range(seed_blocks)]
    digits = (
        asked_of(far_hot, far_pos, far_rows_of, 0, asked)
        + asked_of(first_hot, first_pos, first_rows_of, far_stride, asked)
        + asked_of(seed_hot, seed_pos, seed_rows_of, far_stride + first_cap, asked)
    )
    wishes = (digits[:devices] * 128.0 + digits[devices:]).astype(jnp.int32)
    asks[...] = jnp.clip(wishes, 0, nodes - 1) * 2

    def lay(owner, carry):
        requests[owner] = asks[pl.ds(owner, 1), :]
        return carry

    lax.fori_loop(0, devices, lay, 0)
    met()

    def ask(turn, carry):
        other = lax.rem(me + turn * HOP, devices)
        pltpu.make_async_remote_copy(
            src_ref=requests.at[other],
            dst_ref=arrived.at[me],
            send_sem=ask_send,
            recv_sem=ask_recv,
            device_id=(other,),
            device_id_type=MESH,
        ).start()
        return carry

    lax.fori_loop(1, devices, ask, 0)
    own_ask = pltpu.make_async_copy(requests.at[me], arrived.at[me], small_sem.at[0])
    own_ask.start()

    first_base = far_blocks
    turn_base = first_base + first_blocks
    seed_base = turn_base + first_blocks
    looks, shared = seed_base + first_blocks, far_blocks + first_blocks
    seed_lanes = LANES // FAN1
    far_zero, near_zero = R * far_rows, (R + 1) * near_rows

    def place_of(position, cap):
        return jnp.clip(position.astype(jnp.int32), 0, cap - 1)

    def put(owner, place, kind, rows, stride, zero, store):
        for ref, whose in ((look_own, half), (look_out, 1 - half)):
            at = owner - whose * side
            held = (at >= 0) & (at < side)
            index = at * stride + place
            if kind is not None:
                index = index + kind * rows
            store(ref, jnp.where(held, index, zero) * 2)

    def at_row(row):
        def store(ref, value):
            ref[row] = value

        return store

    def at_seeds(block):
        def store(ref, value):
            for turn in range(FAN1):
                row = block * FAN1 + turn
                if row < first_blocks:
                    lanes = slice(turn * seed_lanes, (turn + 1) * seed_lanes)
                    ref[seed_base + row, 0:1, 0:seed_lanes] = value[:, lanes]

        return store

    for block in range(far_blocks):
        owner = far_owner[0:1, lanes_of[block]]
        place = place_of(far_pos[block], far_cap)
        kind = far_kind[block : block + 1, :]
        put(owner, place, kind, far_rows, far_stride, far_zero, at_row(block))
    for block in range(first_blocks):
        owner = first_owner[0:1, lanes_of[block]]
        place = place_of(first_pos[block], first_cap)
        kind = first_kind[block : block + 1, :] + 1
        put(owner, place, None, near_rows, near_stride, near_zero, at_row(first_base + block))
        put(owner, place, kind, near_rows, near_stride, near_zero, at_row(turn_base + block))
    for block in range(seed_blocks):
        owner = spare_owner[0:1, lanes_of[block]]
        place = place_of(seed_pos[block], seed_cap) + first_cap
        put(owner, place, None, near_rows, near_stride, near_zero, at_seeds(block))
    far_share = shares_of(far_kind[...], FAN2)
    first_share = shares_of(first_kind[...], FAN1)
    for block in range(far_blocks):
        share_own[block] = far_share[block : block + 1, :]
    for block in range(first_blocks):
        share_own[far_blocks + block] = first_share[block : block + 1, :]
    tells = []
    for turn, (source, target) in enumerate(((look_out, look_in), (share_own, share_in))):
        tells.append(
            pltpu.make_async_remote_copy(
                src_ref=source,
                dst_ref=target,
                send_sem=info_send.at[turn],
                recv_sem=info_recv.at[turn],
                device_id=(mirror,),
                device_id_type=MESH,
            )
        )
        tells[-1].start()
    keeps = [
        pltpu.make_async_copy(look_own, look.at[pl.ds(0, looks)], small_sem.at[1]),
        pltpu.make_async_copy(share_own, share.at[pl.ds(0, shared)], small_sem.at[2]),
    ]
    for keep in keeps:
        keep.start()

    part_rows = chunk // 4
    for turn in range(LOADS):
        loads[turn].wait()

        def widen(quarter, carry):
            start = pl.multiple_of(quarter * part_rows, part_rows)
            values = table_half[turn % SLOTS, pl.ds(start, part_rows), :].astype(FULL)
            pair_up(table, pl.multiple_of(2 * (turn * chunk + start), 8), values)
            return carry

        lax.fori_loop(0, 4, widen, 0)
        if turn + SLOTS < LOADS:
            loads[turn + SLOTS].start()
    own_ask.wait()
    others = pl.ds(0, devices - 1)
    pltpu.make_async_copy(requests.at[others], arrived.at[others], ask_send).wait()
    pltpu.make_async_copy(requests.at[others], arrived.at[others], ask_recv).wait()
    moves = []
    for turn in range(2):
        clients = pl.ds(lax.rem(half + turn, 2) * side, side)
        moves.append(
            pltpu.make_async_copy(arrived.at[clients], wanted.at[clients], small_sem.at[5 + turn])
        )
    moves[1].start()
    moves[0].start()
    moves[1].wait()

    def serve(turn, first, stride, send, recv, send_sem, recv_sem):
        whose = lax.rem(half + turn, 2) * side

        def one(step, carry):
            relay = lax.rem(local + step * HOP, side)
            client = whose + relay
            for place in range(stride):
                row = table[pl.ds(wanted[client, 0, first + place], 2), :]
                staging[2 * place : 2 * place + 2, :] = row
            send[client] = paired(staging, 0, stride).astype(HALF)
            where = pl.ds(pl.multiple_of(local * stride, stride), stride)

            @pl.when(step < side)
            def _():
                pltpu.make_async_remote_copy(
                    src_ref=send.at[client],
                    dst_ref=recv.at[turn, where],
                    send_sem=send_sem.at[turn],
                    recv_sem=recv_sem.at[turn],
                    device_id=(half * side + relay,),
                    device_id_type=MESH,
                ).start()

            @pl.when(step == side)
            def _():
                recv[turn, where, :] = send[client]

            return carry

        lax.fori_loop(1, side + 1, one, 0)

    for turn in (1, 0):
        if turn == 0:
            moves[0].wait()
        serve(turn, 0, far_stride, far_send, far_recv, far_send_sem, far_recv_sem)
        serve(turn, far_stride, near_stride, near_send, near_recv, near_send_sem, near_recv_sem)

    far_cast[2 * far_zero : 2 * far_zero + 8, :] = jnp.zeros((8, LANES), FULL)
    near_cast[2 * near_zero : 2 * near_zero + 8, :] = jnp.zeros((8, LANES), FULL)

    lane = lax.broadcasted_iota(jnp.int32, (1, LANES), 1)
    seed_of = lax.broadcasted_iota(jnp.int32, (seed_lanes, LANES), 1) // FAN1
    chosen = (seed_of == lax.broadcasted_iota(jnp.int32, (seed_lanes, LANES), 0)).astype(HALF)
    for block in range(first_blocks):
        kinds = first_kind[block : block + 1, :]
        hot = [
            ((kinds == kind) & (lane % FAN1 == k)).astype(FULL)
            for k in range(FAN1)
            for kind in range(R)
        ]
        kind_columns[block * seed_lanes : (block + 1) * seed_lanes, 0 : FAN1 * R] = lax.dot_general(
            chosen,
            jnp.concatenate(hot, axis=0).astype(HALF),
            (((1,), (1,)), ((), ())),
            preferred_element_type=FULL,
        )

    for copy in weigh:
        copy.wait()
    for tell in tells:
        tell.wait()
    keeps += [
        pltpu.make_async_copy(look_in, look.at[pl.ds(looks, looks)], small_sem.at[3]),
        pltpu.make_async_copy(share_in, share.at[pl.ds(shared, shared)], small_sem.at[4]),
    ]
    for keep in keeps[2:]:
        keep.start()
    for keep in keeps:
        keep.wait()

    def arrive(recv, turn, rows, stride, recv_sem):
        there = pl.ds(0, rows - stride)
        block = recv.at[turn, there]
        pltpu.make_async_copy(block, block, recv_sem.at[turn]).wait()

    def project(recv, turn, rows, cast, first_kind_of, kinds):
        size = rows // 2

        def some(part_of, carry):
            start = pl.multiple_of(part_of * size, size)
            values = recv[turn, pl.ds(start, size), :]
            for kind in range(kinds):
                top = (first_kind_of + kind) * width
                term = jnp.dot(
                    values, first_weights[top : top + width, :], preferred_element_type=FULL
                )
                pair_up(cast, pl.multiple_of(2 * (kind * rows + start), 8), term)
            return carry

        lax.fori_loop(0, 2, some, 0)

    def at(cast, turn, row, lane_of):
        return cast[pl.ds(look[turn * looks + row, 0, lane_of], 2), :]

    def far_sums(turn):
        def one(block, carry):
            for item in range(LANES):
                row, first = (item * FAN2) // LANES, (item * FAN2) % LANES
                total = at(far_cast, turn, block * FAN2 + row, first)
                for k in range(1, FAN2):
                    total = total + at(far_cast, turn, block * FAN2 + row, first + k)
                scale = share[turn * shared + block * FAN2 + row, 0, first]
                far_total[block, 2 * item : 2 * item + 2, :] = scale * total
            return carry

        lax.fori_loop(0, first_blocks, one, 0)

    def sums(turn, block):
        for item in range(LANES):
            place = 2 * item
            staging[place : place + 2, :] = (
                at(near_cast, turn, first_base + block, item)
                + far_total[block, place : place + 2, :]
            )
        for seed in range(seed_lanes):
            total = at(near_cast, turn, seed_base + block, seed)
            for k in range(FAN1):
                item = seed * FAN1 + k
                scale = share[turn * shared + far_blocks + block, 0, item]
                total = total + scale * at(near_cast, turn, turn_base + block, item)
            place = 2 * (LANES + seed)
            staging[place : place + 2, :] = total
        return paired(staging, 0, piece)

    piece = LANES + seed_lanes
    arrive(far_recv, 1, far_rows, far_stride, far_recv_sem)
    project(far_recv, 1, far_rows, far_cast, 1, R)
    far_sums(1)
    arrive(near_recv, 1, near_rows, near_stride, near_recv_sem)
    project(near_recv, 1, near_rows, near_cast, 0, R + 1)

    def mirror_block(block, carry):
        piece_send[block] = sums(1, block).astype(HALF)
        pltpu.make_async_remote_copy(
            src_ref=piece_send.at[block],
            dst_ref=piece_recv.at[block],
            send_sem=piece_send_sem,
            recv_sem=piece_recv_sem.at[block],
            device_id=(mirror,),
            device_id_type=MESH,
        ).start()
        return carry

    lax.fori_loop(0, first_blocks, mirror_block, 0)

    arrive(far_recv, 0, far_rows, far_stride, far_recv_sem)
    project(far_recv, 0, far_rows, far_cast, 1, R)
    far_sums(0)
    arrive(near_recv, 0, near_rows, near_stride, near_recv_sem)
    project(near_recv, 0, near_rows, near_cast, 0, R + 1)

    def own_block(block, carry):
        mine[block] = sums(0, block)
        return carry

    lax.fori_loop(0, first_blocks, own_block, 0)

    def join(block, carry):
        pltpu.make_async_copy(
            piece_recv.at[block], piece_recv.at[block], piece_recv_sem.at[block]
        ).wait()
        value = jnp.maximum(mine[block] + piece_recv[block].astype(FULL), 0.0).astype(HALF)
        for part_of in range(2):
            hop_layer[part_of] = value[:LANES, lanes_of[part_of]].astype(FULL)
        values = [
            jnp.concatenate(
                [hop_layer[part_of, pl.ds(k, seed_lanes, stride=FAN1), :] for part_of in range(2)],
                axis=1,
            )
            for k in range(FAN1)
        ]
        seeds = pl.ds(pl.multiple_of(block * seed_lanes, seed_lanes), seed_lanes)
        columns = kind_columns[seeds, :]
        inputs = [value[LANES:]]
        for kind in range(R):
            hot = [columns[:, k * R + kind : k * R + kind + 1] for k in range(FAN1)]
            portion = 1.0 / jnp.maximum(sum(hot[1:], hot[0]), 1.0)
            mean = (hot[0] * portion) * values[0]
            for k in range(1, FAN1):
                mean = mean + (hot[k] * portion) * values[k]
            inputs.append(mean.astype(HALF))
        second[seeds, :] = jnp.dot(
            jnp.concatenate(inputs, axis=1), second_weights[...], preferred_element_type=FULL
        )
        return carry

    lax.fori_loop(0, first_blocks, join, 0)

    blocks = mask.shape[0]
    positives = blocks * BLOCK
    loss_sum = jnp.zeros((1, 1), FULL)
    edge_sum = jnp.zeros((1, 1), FULL)

    diagonal = lax.broadcasted_iota(jnp.int32, (BLOCK, BLOCK), 0) == lax.broadcasted_iota(
        jnp.int32, (BLOCK, BLOCK), 1
    )
    for block in range(blocks):
        sources = second[block * BLOCK : (block + 1) * BLOCK, :]
        targets = second[positives + block * BLOCK : positives + (block + 1) * BLOCK, :]
        first_neg = 2 * positives + block * NEG
        negatives = second[first_neg : first_neg + NEG, :]
        scores = lax.dot_general(
            jnp.concatenate([targets, negatives], axis=0),
            sources,
            (((1,), (1,)), ((), ())),
            precision=lax.Precision.HIGHEST,
            preferred_element_type=FULL,
        )
        positive = jnp.sum(jnp.where(diagonal, scores[:BLOCK], 0.0), axis=0, keepdims=True)
        negative = scores[BLOCK:]
        top_score = jnp.maximum(positive, jnp.max(negative, axis=0, keepdims=True))
        spread_sum = jnp.exp(positive - top_score) + jnp.sum(
            jnp.exp(negative - top_score), axis=0, keepdims=True
        )
        edge_loss = top_score + jnp.log(spread_sum) - positive
        loss_out[block : block + 1, :] = edge_loss
        counted = mask[block : block + 1, :].astype(FULL)
        loss_sum = loss_sum + jnp.sum(counted * edge_loss, axis=1, keepdims=True)
        edge_sum = edge_sum + jnp.sum(counted, axis=1, keepdims=True)
    part[...] = jnp.where(lane == 0, loss_sum, jnp.where(lane == 1, edge_sum, 0.0))

    def tell_all(turn, carry):
        other = lax.rem(me + turn * HOP, devices)
        pltpu.make_async_remote_copy(
            src_ref=part,
            dst_ref=seen.at[me],
            send_sem=tell_send,
            recv_sem=tell_recv,
            device_id=(other,),
            device_id_type=MESH,
        ).start()
        return carry

    lax.fori_loop(1, devices, tell_all, 0)
    seen[me] = part[...]
    near_side = pl.ds(0, side - 1)
    for turn in range(2):
        sent = far_send.at[near_side]
        pltpu.make_async_copy(sent, sent, far_send_sem.at[turn]).wait()
        sent = near_send.at[near_side]
        pltpu.make_async_copy(sent, sent, near_send_sem.at[turn]).wait()
    pltpu.make_async_copy(piece_send, piece_send, piece_send_sem).wait()
    pltpu.make_async_copy(seen.at[others], seen.at[others], tell_recv).wait()
    pltpu.make_async_copy(seen.at[others], seen.at[others], tell_send).wait()
    total = jnp.sum(seen[...], axis=0)
    mean_out[...] = total[:, 0:1] / jnp.maximum(total[:, 1:2], 1.0)


def fetch(owners, rows, kinds, features, w_first, w_second, mask, caps, counts, devices):
    nodes, width = features.shape
    side = devices // 2
    strides = (round_up(caps[0], 16), round_up(caps[1] + caps[2], 16))
    asked = round_up(sum(strides), LANES)
    far_rows, near_rows = side * strides[0], side * strides[1]
    far_blocks, first_blocks = rows[0].shape[0], rows[1].shape[0]
    looks, shared = far_blocks + 3 * first_blocks, far_blocks + first_blocks
    piece = LANES + LANES // FAN1
    number = jnp.int32
    vmem, anywhere = (pl.BlockSpec(memory_space=space) for space in (pltpu.VMEM, pl.ANY))
    return pl.pallas_call(
        functools.partial(fetch_kernel, devices, caps, strides, counts),
        out_shape=[
            jax.ShapeDtypeStruct(mask.shape, FULL),
            jax.ShapeDtypeStruct((1, 1), FULL),
        ],
        in_specs=[vmem] * 8 + [anywhere] * 3 + [vmem],
        out_specs=[vmem, vmem],
        scratch_shapes=[
            pltpu.VMEM(w_first.shape, HALF),
            pltpu.VMEM(w_second.shape, HALF),
            pltpu.VMEM((1, round_up(counts[2], LANES)), number),
            pltpu.VMEM((1, round_up(counts[2], LANES)), number),
            pltpu.VMEM((SLOTS, nodes // LOADS, width), HALF),
            pltpu.VMEM((2 * nodes, LANES), FULL),
            pltpu.VMEM((devices, asked), number),
            pltpu.VMEM((devices, 1, asked), number),
            pltpu.VMEM((devices, 1, asked), number),
            pltpu.SMEM((devices, 1, asked), number),
            pltpu.VMEM((looks, 1, LANES), number),
            pltpu.VMEM((looks, 1, LANES), number),
            pltpu.VMEM((looks, 1, LANES), number),
            pltpu.VMEM((shared, 1, LANES), FULL),
            pltpu.VMEM((shared, 1, LANES), FULL),
            pltpu.SMEM((2 * looks, 1, LANES), number),
            pltpu.SMEM((2 * shared, 1, LANES), FULL),
            pltpu.VMEM((devices, strides[0], width), HALF),
            pltpu.VMEM((devices, strides[1], width), HALF),
            pltpu.VMEM((2, far_rows, width), HALF),
            pltpu.VMEM((2, near_rows, width), HALF),
            pltpu.VMEM((2 * R * far_rows + 8, LANES), FULL),
            pltpu.VMEM((2 * (R + 1) * near_rows + 8, LANES), FULL),
            pltpu.VMEM((2 * max(sum(strides), piece), LANES), FULL),
            pltpu.VMEM((first_blocks, 2 * LANES, LANES), FULL),
            pltpu.VMEM((first_blocks, piece, width), FULL),
            pltpu.VMEM((2, LANES, LANES), FULL),
            pltpu.VMEM((counts[2], LANES), FULL),
            pltpu.VMEM((first_blocks, piece, width), HALF),
            pltpu.VMEM((first_blocks, piece, width), HALF),
            pltpu.VMEM((counts[2], width), FULL),
            pltpu.VMEM((1, LANES), FULL),
            pltpu.VMEM((devices, 1, LANES), FULL),
            pltpu.SemaphoreType.DMA((LOADS,)),
            pltpu.SemaphoreType.DMA((2,)),
            pltpu.SemaphoreType.DMA((7,)),
            pltpu.SemaphoreType.DMA(()),
            pltpu.SemaphoreType.DMA(()),
        ]
        + [pltpu.SemaphoreType.DMA((2,))] * 6
        + [pltpu.SemaphoreType.DMA(())]
        + [pltpu.SemaphoreType.DMA((first_blocks,))]
        + [pltpu.SemaphoreType.DMA(())] * 2,
        compiler_params=pltpu.CompilerParams(
            collective_id=0, has_side_effects=True, vmem_limit_bytes=67043328
        ),
        name="fetch",
    )(*owners, *rows, *kinds, features, w_first, w_second, mask)


def shards(
    features,
    w_first,
    w_second,
    seed_owner,
    seed_row,
    hop1_owner,
    hop1_row,
    hop1_rel,
    hop2_owner,
    hop2_row,
    hop2_rel,
    edge_mask,
):
    devices = lax.axis_size("dom")
    counts = (hop2_row.shape[0], hop1_row.shape[0], seed_row.shape[0])
    caps = tuple((2 * length + devices - 1) // devices for length in counts)

    owners = [owner.reshape(1, -1) for owner in (hop2_owner, hop1_owner, seed_owner)]
    rows = [hop2_row.reshape(-1, LANES), hop1_row.reshape(-1, LANES), seed_row]
    edge_loss, mean_loss = fetch(
        owners,
        rows,
        [rel.reshape(-1, LANES) for rel in (hop2_rel, hop1_rel)],
        features,
        w_first,
        w_second,
        edge_mask.reshape(-1, BLOCK),
        caps,
        counts,
        devices,
    )
    return (edge_loss.reshape(-1), mean_loss[0, 0])


def solution(mesh):
    placed = (
        P("dom", None),
        P(),
        P(),
        P("dom", None),
        P("dom"),
        P("dom", None),
        P("dom"),
        P("dom"),
        P("dom", None),
        P("dom"),
        P("dom"),
        P("dom"),
    )
    return jax.shard_map(
        shards, mesh=mesh, in_specs=placed, out_specs=(P("dom"), P()), check_vma=False
    )
```

```python
import functools

import jax
import jax.numpy as jnp
from jax import lax
from jax.experimental import pallas as pl
from jax.experimental.pallas import tpu as pltpu
from jax.sharding import PartitionSpec as P

MESH = pl.DeviceIdType.MESH
HOP = 11
LANES = 128
LOADS = 8
SLOTS = 4

R = 4
BLOCK = 128
NEG = 32
FAN1 = 4
FAN2 = 2

HALF, FULL = jnp.bfloat16, jnp.float32


def round_up(value, multiple):
    return (value + multiple - 1) // multiple * multiple


def paired(ref, start, count):
    parts = [ref[pl.ds(start + part, count, stride=2), :] for part in range(2)]
    return jnp.concatenate(parts, axis=1)


def pair_up(ref, start, values):
    count = values.shape[0]
    for part in range(2):
        ref[pl.ds(start + part, count, stride=2), :] = values[:, part * LANES : (part + 1) * LANES]


def greet(devices, me):
    barrier = pltpu.get_barrier_semaphore()

    def hail(step, carry):
        other = lax.rem(me + step, devices)
        pl.semaphore_signal(barrier, inc=1, device_id=(other,), device_id_type=MESH)
        return carry

    lax.fori_loop(1, devices, hail, 0)
    return lambda: pl.semaphore_wait(barrier, devices - 1)


def ranks(devices, owner_ref, blocks):
    lane = lax.broadcasted_iota(jnp.int32, (LANES, 2 * LANES), 1)
    item = lax.broadcasted_iota(jnp.int32, (LANES, 2 * LANES), 0)
    counting = ((item < lane) | (lane >= LANES)).astype(HALF)
    owner_id = lax.broadcasted_iota(jnp.int32, (devices, LANES), 0)
    hots = []
    for block in range(blocks):
        owner = owner_ref[0:1, block * LANES : (block + 1) * LANES]
        hots.append((owner == owner_id).astype(FULL))
    counted = jnp.dot(
        jnp.concatenate(hots, axis=0).astype(HALF), counting, preferred_element_type=FULL
    )
    running = jnp.zeros((devices, LANES), FULL)
    positions = []
    for block in range(blocks):
        mine = counted[block * devices : (block + 1) * devices]
        prior = mine[:, :LANES] + running
        running = running + mine[:, LANES:]
        positions.append(jnp.sum(prior * hots[block], axis=0, keepdims=True))
    return hots, positions


def asked_of(hots, positions, rows, offset, width):
    slot = lax.broadcasted_iota(jnp.int32, (width, LANES), 0).astype(FULL)
    total = None
    for block, (hot, position) in enumerate(zip(hots, positions)):
        row = rows[block]
        high = lax.shift_right_logical(row, 7).astype(FULL)
        low = jnp.bitwise_and(row, 127).astype(FULL)
        digits = jnp.concatenate([hot * high, hot * low], axis=0).astype(HALF)
        placed = (slot == position + float(offset)).astype(FULL).astype(HALF)
        term = lax.dot_general(
            digits, placed, (((1,), (1,)), ((), ())), preferred_element_type=FULL
        )
        total = term if total is None else total + term
    return total


def shares_of(kinds, fan):
    first = lax.broadcasted_iota(jnp.int32, (LANES, LANES), 0) // fan
    second = lax.broadcasted_iota(jnp.int32, (LANES, LANES), 1) // fan
    together = (first == second).astype(HALF)
    count = None
    for kind in range(R):
        same = (kinds == kind).astype(FULL)
        term = same * jnp.dot(same.astype(HALF), together, preferred_element_type=FULL)
        count = term if count is None else count + term
    return 1.0 / jnp.maximum(count, 1.0)


def fetch_kernel(
    devices,
    caps,
    strides,
    counts,
    far_owner,
    first_owner,
    seed_owner,
    far_row,
    first_row,
    seed_row,
    far_kind,
    first_kind,
    features,
    w_first,
    w_second,
    mask,
    loss_out,
    mean_out,
    first_weights,
    second_weights,
    spare_owner,
    spare_row,
    table_half,
    table,
    asks,
    requests,
    arrived,
    wanted,
    look_own,
    look_out,
    look_in,
    share_own,
    share_in,
    look,
    share,
    far_send,
    near_send,
    far_recv,
    near_recv,
    far_cast,
    near_cast,
    staging,
    far_total,
    mine,
    hop_layer,
    kind_columns,
    piece_send,
    piece_recv,
    second,
    part,
    seen,
    load_sem,
    weight_sem,
    small_sem,
    ask_send,
    ask_recv,
    info_send,
    info_recv,
    far_send_sem,
    far_recv_sem,
    near_send_sem,
    near_recv_sem,
    piece_send_sem,
    piece_recv_sem,
    tell_send,
    tell_recv,
):
    me = lax.axis_index("dom")
    side = devices // 2
    plane = side // 2
    half = lax.div(me, side)
    local = lax.rem(me, side)
    mirror = lax.rem(me + side, devices)
    far_count, first_count, seed_count = counts
    width = features.shape[1]
    far_cap, first_cap, seed_cap = caps
    far_stride, near_stride = strides
    far_rows, near_rows = side * far_stride, side * near_stride
    asked = requests.shape[2]
    nodes = features.shape[0]
    chunk = nodes // LOADS
    loads = [
        pltpu.make_async_copy(
            features.at[pl.ds(turn * chunk, chunk)],
            table_half.at[turn % SLOTS],
            load_sem.at[turn],
        )
        for turn in range(LOADS)
    ]
    for load in loads[:SLOTS]:
        load.start()
    weigh = [
        pltpu.make_async_copy(w_first, first_weights, weight_sem.at[0]),
        pltpu.make_async_copy(w_second, second_weights, weight_sem.at[1]),
    ]
    for copy in weigh:
        copy.start()
    met = greet(devices, me)

    spare_owner[...] = jnp.full(spare_owner.shape, -1, jnp.int32)
    spare_row[...] = jnp.zeros(spare_row.shape, jnp.int32)
    spare_owner[0:1, 0:seed_count] = seed_owner[...]
    spare_row[0:1, 0:seed_count] = seed_row[...].reshape(1, seed_count)
    far_blocks, first_blocks = far_row.shape[0], first_row.shape[0]
    seed_blocks = spare_row.shape[1] // LANES
    lanes_of = [slice(block * LANES, (block + 1) * LANES) for block in range(far_blocks)]
    far_hot, far_pos = ranks(devices, far_owner, far_blocks)
    first_hot, first_pos = ranks(devices, first_owner, first_blocks)
    seed_hot, seed_pos = ranks(devices, spare_owner, seed_blocks)
    far_rows_of = [far_row[block : block + 1, :] for block in range(far_blocks)]
    first_rows_of = [first_row[block : block + 1, :] for block in range(first_blocks)]
    seed_rows_of = [spare_row[0:1, lanes_of[block]] for block in range(seed_blocks)]
    digits = (
        asked_of(far_hot, far_pos, far_rows_of, 0, asked)
        + asked_of(first_hot, first_pos, first_rows_of, far_stride, asked)
        + asked_of(seed_hot, seed_pos, seed_rows_of, far_stride + first_cap, asked)
    )
    wishes = (digits[:devices] * 128.0 + digits[devices:]).astype(jnp.int32)
    asks[...] = jnp.clip(wishes, 0, nodes - 1) * 2

    def lay(owner, carry):
        requests[owner] = asks[pl.ds(owner, 1), :]
        return carry

    lax.fori_loop(0, devices, lay, 0)
    met()

    def ask(turn, carry):
        other = lax.rem(me + turn * HOP, devices)
        pltpu.make_async_remote_copy(
            src_ref=requests.at[other],
            dst_ref=arrived.at[me],
            send_sem=ask_send,
            recv_sem=ask_recv,
            device_id=(other,),
            device_id_type=MESH,
        ).start()
        return carry

    lax.fori_loop(1, devices, ask, 0)
    own_ask = pltpu.make_async_copy(requests.at[me], arrived.at[me], small_sem.at[0])
    own_ask.start()

    first_base = far_blocks
    turn_base = first_base + first_blocks
    seed_base = turn_base + first_blocks
    looks, shared = seed_base + first_blocks, far_blocks + first_blocks
    seed_lanes = LANES // FAN1
    far_zero, near_zero = R * far_rows, (R + 1) * near_rows

    def place_of(position, cap):
        return jnp.clip(position.astype(jnp.int32), 0, cap - 1)

    def put(owner, place, kind, rows, stride, zero, store):
        for ref, whose in ((look_own, half), (look_out, 1 - half)):
            at = owner - whose * side
            held = (at >= 0) & (at < side)
            index = at * stride + place
            if kind is not None:
                index = index + kind * rows
            store(ref, jnp.where(held, index, zero) * 2)

    def at_row(row):
        def store(ref, value):
            ref[row] = value

        return store

    def at_seeds(block):
        def store(ref, value):
            for turn in range(FAN1):
                row = block * FAN1 + turn
                if row < first_blocks:
                    lanes = slice(turn * seed_lanes, (turn + 1) * seed_lanes)
                    ref[seed_base + row, 0:1, 0:seed_lanes] = value[:, lanes]

        return store

    for block in range(far_blocks):
        owner = far_owner[0:1, lanes_of[block]]
        place = place_of(far_pos[block], far_cap)
        kind = far_kind[block : block + 1, :]
        put(owner, place, kind, far_rows, far_stride, far_zero, at_row(block))
    for block in range(first_blocks):
        owner = first_owner[0:1, lanes_of[block]]
        place = place_of(first_pos[block], first_cap)
        kind = first_kind[block : block + 1, :] + 1
        put(owner, place, None, near_rows, near_stride, near_zero, at_row(first_base + block))
        put(owner, place, kind, near_rows, near_stride, near_zero, at_row(turn_base + block))
    for block in range(seed_blocks):
        owner = spare_owner[0:1, lanes_of[block]]
        place = place_of(seed_pos[block], seed_cap) + first_cap
        put(owner, place, None, near_rows, near_stride, near_zero, at_seeds(block))
    far_share = shares_of(far_kind[...], FAN2)
    first_share = shares_of(first_kind[...], FAN1)
    for block in range(far_blocks):
        share_own[block] = far_share[block : block + 1, :]
    for block in range(first_blocks):
        share_own[far_blocks + block] = first_share[block : block + 1, :]
    tells = []
    for turn, (source, target) in enumerate(((look_out, look_in), (share_own, share_in))):
        tells.append(
            pltpu.make_async_remote_copy(
                src_ref=source,
                dst_ref=target,
                send_sem=info_send.at[turn],
                recv_sem=info_recv.at[turn],
                device_id=(mirror,),
                device_id_type=MESH,
            )
        )
        tells[-1].start()
    keeps = [
        pltpu.make_async_copy(look_own, look.at[pl.ds(0, looks)], small_sem.at[1]),
        pltpu.make_async_copy(share_own, share.at[pl.ds(0, shared)], small_sem.at[2]),
    ]
    for keep in keeps:
        keep.start()

    part_rows = chunk // 4
    for turn in range(LOADS):
        loads[turn].wait()

        def widen(quarter, carry):
            start = pl.multiple_of(quarter * part_rows, part_rows)
            values = table_half[turn % SLOTS, pl.ds(start, part_rows), :].astype(FULL)
            pair_up(table, pl.multiple_of(2 * (turn * chunk + start), 8), values)
            return carry

        lax.fori_loop(0, 4, widen, 0)
        if turn + SLOTS < LOADS:
            loads[turn + SLOTS].start()
    own_ask.wait()
    others = pl.ds(0, devices - 1)
    pltpu.make_async_copy(requests.at[others], arrived.at[others], ask_send).wait()
    pltpu.make_async_copy(requests.at[others], arrived.at[others], ask_recv).wait()
    moves = []
    for turn in range(2):
        clients = pl.ds(lax.rem(half + turn, 2) * side, side)
        moves.append(
            pltpu.make_async_copy(arrived.at[clients], wanted.at[clients], small_sem.at[5 + turn])
        )
    moves[1].start()
    moves[0].start()
    moves[1].wait()

    def serve(turn, first, stride, send, recv, send_sem, recv_sem):
        whose = lax.rem(half + turn, 2) * side

        def one(step, carry):
            across = lax.rem(step, 2)
            its_plane = lax.rem(lax.div(local, plane) + across, 2)
            relay = its_plane * plane + lax.rem(local + lax.div(step, 2), plane)
            client = whose + relay
            for place in range(stride):
                row = table[pl.ds(wanted[client, 0, first + place], 2), :]
                staging[2 * place : 2 * place + 2, :] = row
            send[client] = paired(staging, 0, stride).astype(HALF)
            where = pl.ds(pl.multiple_of(local * stride, stride), stride)

            @pl.when(step < side)
            def _():
                pltpu.make_async_remote_copy(
                    src_ref=send.at[client],
                    dst_ref=recv.at[turn, where],
                    send_sem=send_sem.at[turn],
                    recv_sem=recv_sem.at[turn, across],
                    device_id=(half * side + relay,),
                    device_id_type=MESH,
                ).start()

            @pl.when(step == side)
            def _():
                recv[turn, where, :] = send[client]

            return carry

        lax.fori_loop(1, side + 1, one, 0)

    for turn in (1, 0):
        if turn == 0:
            moves[0].wait()
        serve(turn, 0, far_stride, far_send, far_recv, far_send_sem, far_recv_sem)
        serve(turn, far_stride, near_stride, near_send, near_recv, near_send_sem, near_recv_sem)

    far_cast[2 * far_zero : 2 * far_zero + 8, :] = jnp.zeros((8, LANES), FULL)
    near_cast[2 * near_zero : 2 * near_zero + 8, :] = jnp.zeros((8, LANES), FULL)

    lane = lax.broadcasted_iota(jnp.int32, (1, LANES), 1)
    seed_of = lax.broadcasted_iota(jnp.int32, (seed_lanes, LANES), 1) // FAN1
    chosen = (seed_of == lax.broadcasted_iota(jnp.int32, (seed_lanes, LANES), 0)).astype(HALF)
    for block in range(first_blocks):
        kinds = first_kind[block : block + 1, :]
        hot = [
            ((kinds == kind) & (lane % FAN1 == k)).astype(FULL)
            for k in range(FAN1)
            for kind in range(R)
        ]
        kind_columns[block * seed_lanes : (block + 1) * seed_lanes, 0 : FAN1 * R] = lax.dot_general(
            chosen,
            jnp.concatenate(hot, axis=0).astype(HALF),
            (((1,), (1,)), ((), ())),
            preferred_element_type=FULL,
        )

    for copy in weigh:
        copy.wait()
    for tell in tells:
        tell.wait()
    keeps += [
        pltpu.make_async_copy(look_in, look.at[pl.ds(looks, looks)], small_sem.at[3]),
        pltpu.make_async_copy(share_in, share.at[pl.ds(shared, shared)], small_sem.at[4]),
    ]
    for keep in keeps[2:]:
        keep.start()
    for keep in keeps:
        keep.wait()

    def arrive(recv, turn, across, stride, recv_sem):
        there = pl.ds(0, (plane - 1 + across) * stride)
        block = recv.at[turn, there]
        pltpu.make_async_copy(block, block, recv_sem.at[turn, across]).wait()

    def project(recv, turn, rows, cast, first_kind_of, kinds, stride, recv_sem):
        size = rows // 2

        for across in range(2):
            arrive(recv, turn, across, stride, recv_sem)
            part_of = lax.rem(lax.div(local, plane) + across, 2)
            start = pl.multiple_of(part_of * size, size)
            values = recv[turn, pl.ds(start, size), :]
            for kind in range(kinds):
                top = (first_kind_of + kind) * width
                term = jnp.dot(
                    values, first_weights[top : top + width, :], preferred_element_type=FULL
                )
                pair_up(cast, pl.multiple_of(2 * (kind * rows + start), 8), term)

    def at(cast, turn, row, lane_of):
        return cast[pl.ds(look[turn * looks + row, 0, lane_of], 2), :]

    def far_sums(turn):
        def one(block, carry):
            for item in range(LANES):
                row, first = (item * FAN2) // LANES, (item * FAN2) % LANES
                total = at(far_cast, turn, block * FAN2 + row, first)
                for k in range(1, FAN2):
                    total = total + at(far_cast, turn, block * FAN2 + row, first + k)
                scale = share[turn * shared + block * FAN2 + row, 0, first]
                far_total[block, 2 * item : 2 * item + 2, :] = scale * total
            return carry

        lax.fori_loop(0, first_blocks, one, 0)

    def sums(turn, block):
        for item in range(LANES):
            place = 2 * item
            staging[place : place + 2, :] = (
                at(near_cast, turn, first_base + block, item)
                + far_total[block, place : place + 2, :]
            )
        for seed in range(seed_lanes):
            total = at(near_cast, turn, seed_base + block, seed)
            for k in range(FAN1):
                item = seed * FAN1 + k
                scale = share[turn * shared + far_blocks + block, 0, item]
                total = total + scale * at(near_cast, turn, turn_base + block, item)
            place = 2 * (LANES + seed)
            staging[place : place + 2, :] = total
        return paired(staging, 0, piece)

    piece = LANES + seed_lanes
    project(far_recv, 1, far_rows, far_cast, 1, R, far_stride, far_recv_sem)
    far_sums(1)
    project(near_recv, 1, near_rows, near_cast, 0, R + 1, near_stride, near_recv_sem)

    def mirror_block(block, carry):
        piece_send[block] = sums(1, block).astype(HALF)
        pltpu.make_async_remote_copy(
            src_ref=piece_send.at[block],
            dst_ref=piece_recv.at[block],
            send_sem=piece_send_sem,
            recv_sem=piece_recv_sem.at[block],
            device_id=(mirror,),
            device_id_type=MESH,
        ).start()
        return carry

    lax.fori_loop(0, first_blocks, mirror_block, 0)

    project(far_recv, 0, far_rows, far_cast, 1, R, far_stride, far_recv_sem)
    far_sums(0)
    project(near_recv, 0, near_rows, near_cast, 0, R + 1, near_stride, near_recv_sem)

    def own_block(block, carry):
        mine[block] = sums(0, block)
        return carry

    lax.fori_loop(0, first_blocks, own_block, 0)

    def join(block, carry):
        pltpu.make_async_copy(
            piece_recv.at[block], piece_recv.at[block], piece_recv_sem.at[block]
        ).wait()
        value = jnp.maximum(mine[block] + piece_recv[block].astype(FULL), 0.0).astype(HALF)
        for part_of in range(2):
            hop_layer[part_of] = value[:LANES, lanes_of[part_of]].astype(FULL)
        values = [
            jnp.concatenate(
                [hop_layer[part_of, pl.ds(k, seed_lanes, stride=FAN1), :] for part_of in range(2)],
                axis=1,
            )
            for k in range(FAN1)
        ]
        seeds = pl.ds(pl.multiple_of(block * seed_lanes, seed_lanes), seed_lanes)
        columns = kind_columns[seeds, :]
        inputs = [value[LANES:]]
        for kind in range(R):
            hot = [columns[:, k * R + kind : k * R + kind + 1] for k in range(FAN1)]
            portion = 1.0 / jnp.maximum(sum(hot[1:], hot[0]), 1.0)
            mean = (hot[0] * portion) * values[0]
            for k in range(1, FAN1):
                mean = mean + (hot[k] * portion) * values[k]
            inputs.append(mean.astype(HALF))
        second[seeds, :] = jnp.dot(
            jnp.concatenate(inputs, axis=1), second_weights[...], preferred_element_type=FULL
        )
        return carry

    lax.fori_loop(0, first_blocks, join, 0)

    blocks = mask.shape[0]
    positives = blocks * BLOCK
    loss_sum = jnp.zeros((1, 1), FULL)
    edge_sum = jnp.zeros((1, 1), FULL)

    diagonal = lax.broadcasted_iota(jnp.int32, (BLOCK, BLOCK), 0) == lax.broadcasted_iota(
        jnp.int32, (BLOCK, BLOCK), 1
    )
    for block in range(blocks):
        sources = second[block * BLOCK : (block + 1) * BLOCK, :]
        targets = second[positives + block * BLOCK : positives + (block + 1) * BLOCK, :]
        first_neg = 2 * positives + block * NEG
        negatives = second[first_neg : first_neg + NEG, :]
        scores = lax.dot_general(
            jnp.concatenate([targets, negatives], axis=0),
            sources,
            (((1,), (1,)), ((), ())),
            precision=lax.Precision.HIGHEST,
            preferred_element_type=FULL,
        )
        positive = jnp.sum(jnp.where(diagonal, scores[:BLOCK], 0.0), axis=0, keepdims=True)
        negative = scores[BLOCK:]
        top_score = jnp.maximum(positive, jnp.max(negative, axis=0, keepdims=True))
        spread_sum = jnp.exp(positive - top_score) + jnp.sum(
            jnp.exp(negative - top_score), axis=0, keepdims=True
        )
        edge_loss = top_score + jnp.log(spread_sum) - positive
        loss_out[block : block + 1, :] = edge_loss
        counted = mask[block : block + 1, :].astype(FULL)
        loss_sum = loss_sum + jnp.sum(counted * edge_loss, axis=1, keepdims=True)
        edge_sum = edge_sum + jnp.sum(counted, axis=1, keepdims=True)
    part[...] = jnp.where(lane == 0, loss_sum, jnp.where(lane == 1, edge_sum, 0.0))

    def tell_all(turn, carry):
        other = lax.rem(me + turn * HOP, devices)
        pltpu.make_async_remote_copy(
            src_ref=part,
            dst_ref=seen.at[me],
            send_sem=tell_send,
            recv_sem=tell_recv,
            device_id=(other,),
            device_id_type=MESH,
        ).start()
        return carry

    lax.fori_loop(1, devices, tell_all, 0)
    seen[me] = part[...]
    near_side = pl.ds(0, side - 1)
    for turn in range(2):
        sent = far_send.at[near_side]
        pltpu.make_async_copy(sent, sent, far_send_sem.at[turn]).wait()
        sent = near_send.at[near_side]
        pltpu.make_async_copy(sent, sent, near_send_sem.at[turn]).wait()
    pltpu.make_async_copy(piece_send, piece_send, piece_send_sem).wait()
    pltpu.make_async_copy(seen.at[others], seen.at[others], tell_recv).wait()
    pltpu.make_async_copy(seen.at[others], seen.at[others], tell_send).wait()
    total = jnp.sum(seen[...], axis=0)
    mean_out[...] = total[:, 0:1] / jnp.maximum(total[:, 1:2], 1.0)


def fetch(owners, rows, kinds, features, w_first, w_second, mask, caps, counts, devices):
    nodes, width = features.shape
    side = devices // 2
    strides = (round_up(caps[0], 16), round_up(caps[1] + caps[2], 16))
    asked = round_up(sum(strides), LANES)
    far_rows, near_rows = side * strides[0], side * strides[1]
    far_blocks, first_blocks = rows[0].shape[0], rows[1].shape[0]
    looks, shared = far_blocks + 3 * first_blocks, far_blocks + first_blocks
    piece = LANES + LANES // FAN1
    number = jnp.int32
    vmem, anywhere = (pl.BlockSpec(memory_space=space) for space in (pltpu.VMEM, pl.ANY))
    return pl.pallas_call(
        functools.partial(fetch_kernel, devices, caps, strides, counts),
        out_shape=[
            jax.ShapeDtypeStruct(mask.shape, FULL),
            jax.ShapeDtypeStruct((1, 1), FULL),
        ],
        in_specs=[vmem] * 8 + [anywhere] * 3 + [vmem],
        out_specs=[vmem, vmem],
        scratch_shapes=[
            pltpu.VMEM(w_first.shape, HALF),
            pltpu.VMEM(w_second.shape, HALF),
            pltpu.VMEM((1, round_up(counts[2], LANES)), number),
            pltpu.VMEM((1, round_up(counts[2], LANES)), number),
            pltpu.VMEM((SLOTS, nodes // LOADS, width), HALF),
            pltpu.VMEM((2 * nodes, LANES), FULL),
            pltpu.VMEM((devices, asked), number),
            pltpu.VMEM((devices, 1, asked), number),
            pltpu.VMEM((devices, 1, asked), number),
            pltpu.SMEM((devices, 1, asked), number),
            pltpu.VMEM((looks, 1, LANES), number),
            pltpu.VMEM((looks, 1, LANES), number),
            pltpu.VMEM((looks, 1, LANES), number),
            pltpu.VMEM((shared, 1, LANES), FULL),
            pltpu.VMEM((shared, 1, LANES), FULL),
            pltpu.SMEM((2 * looks, 1, LANES), number),
            pltpu.SMEM((2 * shared, 1, LANES), FULL),
            pltpu.VMEM((devices, strides[0], width), HALF),
            pltpu.VMEM((devices, strides[1], width), HALF),
            pltpu.VMEM((2, far_rows, width), HALF),
            pltpu.VMEM((2, near_rows, width), HALF),
            pltpu.VMEM((2 * R * far_rows + 8, LANES), FULL),
            pltpu.VMEM((2 * (R + 1) * near_rows + 8, LANES), FULL),
            pltpu.VMEM((2 * max(sum(strides), piece), LANES), FULL),
            pltpu.VMEM((first_blocks, 2 * LANES, LANES), FULL),
            pltpu.VMEM((first_blocks, piece, width), FULL),
            pltpu.VMEM((2, LANES, LANES), FULL),
            pltpu.VMEM((counts[2], LANES), FULL),
            pltpu.VMEM((first_blocks, piece, width), HALF),
            pltpu.VMEM((first_blocks, piece, width), HALF),
            pltpu.VMEM((counts[2], width), FULL),
            pltpu.VMEM((1, LANES), FULL),
            pltpu.VMEM((devices, 1, LANES), FULL),
            pltpu.SemaphoreType.DMA((LOADS,)),
            pltpu.SemaphoreType.DMA((2,)),
            pltpu.SemaphoreType.DMA((7,)),
            pltpu.SemaphoreType.DMA(()),
            pltpu.SemaphoreType.DMA(()),
        ]
        + [pltpu.SemaphoreType.DMA((2,))] * 2
        + [pltpu.SemaphoreType.DMA((2,)), pltpu.SemaphoreType.DMA((2, 2))] * 2
        + [pltpu.SemaphoreType.DMA(())]
        + [pltpu.SemaphoreType.DMA((first_blocks,))]
        + [pltpu.SemaphoreType.DMA(())] * 2,
        compiler_params=pltpu.CompilerParams(
            collective_id=0, has_side_effects=True, vmem_limit_bytes=67043328
        ),
        name="fetch",
    )(*owners, *rows, *kinds, features, w_first, w_second, mask)


def shards(
    features,
    w_first,
    w_second,
    seed_owner,
    seed_row,
    hop1_owner,
    hop1_row,
    hop1_rel,
    hop2_owner,
    hop2_row,
    hop2_rel,
    edge_mask,
):
    devices = lax.axis_size("dom")
    counts = (hop2_row.shape[0], hop1_row.shape[0], seed_row.shape[0])
    caps = tuple((2 * length + devices - 1) // devices for length in counts)

    owners = [owner.reshape(1, -1) for owner in (hop2_owner, hop1_owner, seed_owner)]
    rows = [hop2_row.reshape(-1, LANES), hop1_row.reshape(-1, LANES), seed_row]
    edge_loss, mean_loss = fetch(
        owners,
        rows,
        [rel.reshape(-1, LANES) for rel in (hop2_rel, hop1_rel)],
        features,
        w_first,
        w_second,
        edge_mask.reshape(-1, BLOCK),
        caps,
        counts,
        devices,
    )
    return (edge_loss.reshape(-1), mean_loss[0, 0])


def solution(mesh):
    placed = (
        P("dom", None),
        P(),
        P(),
        P("dom", None),
        P("dom"),
        P("dom", None),
        P("dom"),
        P("dom"),
        P("dom", None),
        P("dom"),
        P("dom"),
        P("dom"),
    )
    return jax.shard_map(
        shards, mesh=mesh, in_specs=placed, out_specs=(P("dom"), P()), check_vma=False
    )
```
